256 devices in a mesh: comp: 2 (over z_hi), lat: 8 (over z_lo, core), lon: 16 (over y, x).
Axes of the slice: x: 4, y: 4, z: 8 (z_hi: 2, z_lo: 4; z = z_hi * 4 + z_lo), core: 2. Of those that a mesh axis runs over, the one named last changes fastest.
Arguments:
- fields: float32 [2, 7, 16384, 256], P('comp', None, ('lat', 'lon')), may hold values from -4 to 4, as said below
- block_owner: int32 [16384], P(('lat', 'lon')), may hold values from 0 to 16383, as said below
- ice_covered: int32 [16384], P(('lat', 'lon')), may hold values 0 or 1
- land_mask: int32 [16384, 256], P(('lat', 'lon')), may hold values 0 or 1
Outputs:
- coupled_out: float32 [2, 2, 16384, 256], P('comp', None, ('lat', 'lon'))
The draws below stay inside these ranges and needn't reach their ends.
Inputs may be any that keep to these rules, and one draw needn't show every extreme that they name: `block_owner`: every block id appears once. Slot d of lat+lon index o holds a block of the ice tile of index d, that is an id from d * 128 to d * 128 + 127. `fields`: ocean channels: winds within 4, currents within 1.5, tilts within 1, air density 0.9 to 1.3; ice channels: velocities within 1.5, mass 0.5 to 4, concentration 0.05 to 1, stresses within 1.5.
All inputs are finite; a program needn't handle non-finite values.
Results may differ from the reference program's by a relative error of at most 0.00002.
Values sent between devices are 32-bit elements.
A program may use at most 64 MiB of HBM per device.

```python
import jax
import jax.numpy as jnp

KB = 128
GX = 1
BY = 2
BX = 128
NSUB = 4
NBALL = 16384
CELLS = 256
N_LAT = 8
N_LON = 16


def clipped_normal(subkey, scale, limit):
    return jnp.clip(scale * jax.random.normal(subkey, (NBALL, CELLS), jnp.float32), -limit, limit)


def uniform_draw(subkey, low, high):
    return jax.random.uniform(subkey, (NBALL, CELLS), jnp.float32, low, high)


def draw_fields(key, part):
    subkeys = jax.random.split(jax.random.fold_in(key, 11), 14)
    wind = [clipped_normal(subkeys[0], 1.5, 4.0), clipped_normal(subkeys[1], 1.5, 4.0)]
    current = [clipped_normal(subkeys[2], 0.5, 1.5), clipped_normal(subkeys[3], 0.5, 1.5)]
    tilt = [clipped_normal(subkeys[4], 0.3, 1.0), clipped_normal(subkeys[5], 0.3, 1.0)]
    drift = [clipped_normal(subkeys[7], 0.5, 1.5), clipped_normal(subkeys[8], 0.5, 1.5)]
    concentration = uniform_draw(subkeys[10], 0.05, 1.0)
    stresses = [clipped_normal(subkeys[11], 0.5, 1.5), clipped_normal(subkeys[12], 0.5, 1.5), clipped_normal(subkeys[13], 0.5, 1.5)]
    density = uniform_draw(subkeys[6], 0.9, 1.3)
    ice_mass = jnp.exp(uniform_draw(subkeys[9], jnp.log(0.5), jnp.log(4.0)))
    ocean = jnp.stack(wind + current + tilt + [density])
    sea_ice = jnp.stack(drift + [ice_mass, concentration] + stresses)
    return jnp.stack([ocean, sea_ice]).astype(jnp.float32)


def draw_block_owner(key, part):
    devices = N_LAT * N_LON
    per_peer = KB // devices
    subkeys = jax.random.split(jax.random.fold_in(key, 5), devices)
    orders = jax.vmap(lambda subkey: jax.random.permutation(subkey, KB))(subkeys)
    ids = orders.astype(jnp.int32) + (jnp.arange(devices, dtype=jnp.int32) * KB)[:, None]
    ids = ids.reshape(devices, devices, per_peer).transpose(1, 0, 2)
    return ids.reshape(devices * KB).astype(jnp.int32)


def plant(array, key, smallest, largest):
    extent = array.shape
    place = [jax.random.randint(jax.random.fold_in(key, axis), (), 0, extent[axis]) for axis in range(len(extent))]
    array = array.at[tuple(place)].set(smallest)
    longest = extent.index(max(extent))
    place[longest] = (place[longest] + 1) % extent[longest]
    return array.at[tuple(place)].set(largest)


def setup_inputs(seed: int = 0) -> dict:
    streams_of = jax.random.split(jax.random.key(seed), 5)
    fields = draw_fields(jax.random.fold_in(streams_of[4], 71), 0)
    block_owner = draw_block_owner(jax.random.fold_in(streams_of[4], 71), 0)
    ice_covered = plant((jax.random.randint(streams_of[2], (NBALL,), 0, 4) < 3).astype(jnp.int32), jax.random.fold_in(streams_of[2], 1), 0, 1)
    land_mask = plant((jax.random.randint(streams_of[3], (NBALL, CELLS), 0, 8) < 1).astype(jnp.int32), jax.random.fold_in(streams_of[3], 1), 0, 1)
    return dict(fields=fields, block_owner=block_owner, ice_covered=ice_covered, land_mask=land_mask)


CD_ICE = 0.1
CW = 1.5
CSTAR = 2.0
ECC2 = 4.0
DMIN2 = 0.25
RELAX = 0.5
DTE = 0.5
CORIO = 0.3
MASS_FLOOR = 0.5
DRAG_FLOOR = 0.1

def air_stress(ocean):
    wind_x, wind_y, current_x, current_y, tilt_x, tilt_y, density = ocean
    speed_ice = jnp.sqrt(wind_x * wind_x + wind_y * wind_y + 1.0)
    scale_ice = density * CD_ICE * speed_ice
    rel_x = wind_x - current_x
    rel_y = wind_y - current_y
    speed_open = jnp.sqrt(rel_x * rel_x + rel_y * rel_y + 1.0)
    scale_open = density * (0.1 + 0.05 * speed_open) * speed_open
    outbound = jnp.stack([scale_ice * wind_x, scale_ice * wind_y, current_x, current_y, tilt_x, tilt_y])
    open_stress = jnp.stack([scale_open * rel_x, scale_open * rel_y])
    return (outbound, open_stress)

def prepare(ice_tile, forcing, active):
    ice_mass = ice_tile[2]
    concentration = ice_tile[3]
    strength = ice_mass * jnp.exp(CSTAR * (concentration - 1.0)) * active
    drag_base = CW * concentration * active
    push_x = active * (concentration * forcing[0] - ice_mass * forcing[4])
    push_y = active * (concentration * forcing[1] - ice_mass * forcing[5])
    return jnp.stack([strength, ice_mass, drag_base, push_x, push_y, forcing[2], forcing[3], active])

def subcycle(ice_state, statics):
    east_vel, north_vel, stress_one, stress_two, stress_three = ice_state
    strength = statics[0]
    east_base = east_vel[:-1, :-1]
    north_base = north_vel[:-1, :-1]
    strain_xx = east_vel[:-1, 1:] - east_base
    strain_yy = north_vel[1:, :-1] - north_base
    shear = east_vel[1:, :-1] - east_base + (north_vel[:-1, 1:] - north_base)
    divergence = strain_xx + strain_yy
    tension = strain_xx - strain_yy
    delta_norm = jnp.sqrt(divergence * divergence + (tension * tension + shear * shear) / ECC2 + DMIN2)
    viscosity = strength[:-1, :-1] / delta_norm
    stress_sum = (stress_one[:-1, :-1] + RELAX * viscosity * (divergence - delta_norm)) / (1.0 + RELAX)
    stress_diff = (stress_two[:-1, :-1] + RELAX * viscosity * tension / ECC2) / (1.0 + RELAX)
    stress_shear = (stress_three[:-1, :-1] + RELAX * viscosity * shear / (2.0 * ECC2)) / (1.0 + RELAX)
    stress_xx = 0.5 * (stress_sum + stress_diff)
    stress_yy = 0.5 * (stress_sum - stress_diff)
    force_x = stress_xx[1:, 1:] - stress_xx[1:, :-1] + (stress_shear[1:, 1:] - stress_shear[:-1, 1:])
    force_y = stress_shear[1:, 1:] - stress_shear[1:, :-1] + (stress_yy[1:, 1:] - stress_yy[:-1, 1:])
    trimmed = statics[:, 1:-1, 1:-1]
    strength, ice_mass, drag_base, push_x, push_y, current_x, current_y, active = trimmed
    east_old = east_vel[1:-1, 1:-1]
    north_old = north_vel[1:-1, 1:-1]
    diff_x = current_x - east_old
    diff_y = current_y - north_old
    drag_coef = drag_base * jnp.sqrt(diff_x * diff_x + diff_y * diff_y + DRAG_FLOOR)
    denominator = jnp.maximum(ice_mass, MASS_FLOOR) / DTE + drag_coef
    east_new = active * (ice_mass / DTE * east_old + force_x + push_x + drag_coef * current_x + CORIO * ice_mass * north_old) / denominator
    north_new = active * (ice_mass / DTE * north_old + force_y + push_y + drag_coef * current_y - CORIO * ice_mass * east_old) / denominator
    new_state = jnp.stack([east_new, north_new, stress_sum[1:, 1:], stress_diff[1:, 1:], stress_shear[1:, 1:]])
    return (new_state, trimmed)

def give_back(ice_state, statics):
    east_vel = ice_state[0]
    north_vel = ice_state[1]
    drag_base = statics[2]
    current_x = statics[5]
    current_y = statics[6]
    diff_x = east_vel - current_x
    diff_y = north_vel - current_y
    factor = drag_base * jnp.sqrt(diff_x * diff_x + diff_y * diff_y + DRAG_FLOOR)
    return jnp.stack([factor * diff_x, factor * diff_y, drag_base / CW])

def to_grid(blocks):
    channels = blocks.shape[0]
    arranged = blocks.reshape(channels, N_LAT, N_LON, KB // GX, GX, BY, BX)
    arranged = arranged.transpose(0, 1, 3, 5, 2, 4, 6)
    return arranged.reshape(channels, N_LAT * (KB // GX) * BY, N_LON * GX * BX)

def from_grid(values):
    channels = values.shape[0]
    arranged = values.reshape(channels, N_LAT, KB // GX, BY, N_LON, GX, BX)
    arranged = arranged.transpose(0, 1, 4, 2, 5, 3, 6)
    return arranged.reshape(channels, N_LAT * N_LON * KB, BY * BX)

def extend_grid(values, width):
    values = jnp.concatenate([values[..., -width:], values, values[..., :width]], axis=-1)
    return jnp.pad(values, ((0, 0), (width, width), (0, 0)))

def reference(fields, block_owner, ice_covered, land_mask):
    outbound, open_stress = air_stress(fields[0])
    geographic = jnp.zeros_like(outbound).at[:, block_owner].set(outbound)
    forcing = to_grid(geographic)
    ice_tile = to_grid(fields[1])
    covered = ice_covered.astype(jnp.float32)[:, None] * (1 - land_mask).astype(jnp.float32)
    active = to_grid(covered[None])[0]
    statics = prepare(ice_tile, forcing, active)
    ice_state = jnp.stack([ice_tile[0], ice_tile[1], ice_tile[4], ice_tile[5], ice_tile[6]])
    ice_state = extend_grid(ice_state, NSUB)
    statics = extend_grid(statics, NSUB)
    for repeat in range(NSUB):
        ice_state, statics = subcycle(ice_state, statics)
    returned = from_grid(give_back(ice_state, statics))
    received_back = returned[:, block_owner]
    ocean_out = received_back[:2] + (1.0 - received_back[2]) * open_stress
    ice_out = from_grid(ice_state[:2])
    return jnp.stack([ocean_out, ice_out])
```

```python
import functools

import jax
import jax.numpy as jnp
from jax import lax
from jax.experimental import pallas as pl
from jax.experimental.pallas import tpu as pltpu
from jax.sharding import PartitionSpec as P


NSUB = 4
NLAT = 8
NLON = 16
NT = NLAT * NLON
TOP = 16
ROWS = 160
MESH = pl.DeviceIdType.MESH
HIGHEST = lax.Precision.HIGHEST
F32 = jnp.float32

U, V, S1, S2, S12, STR, MASS, DRAG, ACT, CX, CY, PX, PY = range(13)
GROUP_ICE = (U, V, MASS, DRAG, S1, S2, S12, ACT)
GROUP_CUR = (CX, CY)
GROUP_PUSH = (PX, PY)


def lanes_of(shape):
    return lax.broadcasted_iota(jnp.int32, shape, len(shape) - 1)


def root(x):
    return x * lax.rsqrt(x)


def kernel(
    f_ref, own_ref, cov_ref, land_ref, out_ref,
    ids, sa, ra, sb, rb, x, act, gat, opn, outb, qmat,
    ss1, sn1, hs1, hn1, pk1, pw1, pe1,
    ss2, sn2, hs2, hn2, pk2, pw2, pe2,
    ss3, sn3, hs3, hn3, pk3, pw3, pe3,
    id_send, id_recv, sa_sem, ra_sem, sb_sem, rb_sem, h_send, h_recv,
):
    comp = lax.axis_index("comp")
    la = lax.axis_index("lat")
    lo = lax.axis_index("lon")
    me = la * NLON + lo
    barrier = pltpu.get_barrier_semaphore()
    sa2, ra2, sb2, rb2 = (r.reshape(4 * NT, 128) for r in (sa, ra, sb, rb))

    def target(chunk, j):
        half = lax.rem(lo // 8 + chunk // 2, 2)
        core = lax.rem(lax.rem(la, 2) + chunk % 2, 2)
        level = lax.rem(la // 2 + lax.rem(j, 4), 4)
        column = lax.rem(lax.rem(lo, 8) + j // 4, 8)
        return 2 * level + core, 8 * half + column

    def send_chunk(src, dst, send_sem, recv_sem, chunk, other):
        def body(j, carry):
            tla, tlo = target(chunk, j)
            t = tla * NLON + tlo
            pltpu.make_async_remote_copy(
                src_ref=src.at[pl.ds(4 * t, 4)],
                dst_ref=dst.at[pl.ds(4 * me, 4)],
                send_sem=send_sem,
                recv_sem=recv_sem.at[chunk],
                device_id=(other, tla, tlo),
                device_id_type=MESH,
            ).start()
            return carry

        lax.fori_loop(0, 32, body, 0)

    def wait_bytes(ref, sem):
        pltpu.make_async_copy(ref, ref, sem).wait()

    def wait_chunk(dst, recv_sem, chunk):
        wait_bytes(dst.at[pl.ds(0, 128)], recv_sem.at[chunk])

    @pl.when(comp == 0)
    def _():
        def greet(k, carry):
            t = lax.rem(me + k, NT)
            pl.semaphore_signal(barrier, inc=1, device_id=(1, t // NLON, lax.rem(t, NLON)), device_id_type=MESH)
            return carry

        lax.fori_loop(0, NT, greet, 0)
        for ch in range(2):
            for par in range(2):
                sa2[pl.ds(2 * ch + par, NT, stride=4), :] = f_ref[2 + ch, :, pl.ds(128 * par, 128)]
        pl.semaphore_wait(barrier, NT)
        for chunk in range(4):
            send_chunk(sa, ra, sa_sem, ra_sem, chunk, 1)

        def air(k, carry):
            rows = pl.ds(pl.multiple_of(8 * k, 8), 8)
            wx, wy, cx, cy, rho = (f_ref[i, rows, :] for i in (0, 1, 2, 3, 6))
            scale = rho * 0.1 * root(wx * wx + wy * wy + 1.0)
            outb[0, rows, :] = scale * wx
            outb[1, rows, :] = scale * wy
            rx = wx - cx
            ry = wy - cy
            speed = root(rx * rx + ry * ry + 1.0)
            scale = rho * (0.1 + 0.05 * speed) * speed
            opn[0, rows, :] = scale * rx
            opn[1, rows, :] = scale * ry
            return carry

        lax.fori_loop(0, 16, air, 0)

        for chunk in range(4):
            wait_chunk(ra, ra_sem, chunk)

            def push(level, carry):
                tla, tlo = target(chunk, level)
                base = tla * NLON + tlo // 8 * 8
                rows = pl.ds(pl.multiple_of(base, 8), 8)
                for par in range(2):
                    lanes = pl.ds(128 * par, 128)
                    conc = ra2[pl.ds(4 * base + par, 8, stride=4), :]
                    mass = ra2[pl.ds(4 * base + 2 + par, 8, stride=4), :]
                    for ch in range(2):
                        sb2[pl.ds(4 * base + 2 * ch + par, 8, stride=4), :] = (
                            conc * outb[ch, rows, lanes] - mass * f_ref[4 + ch, rows, lanes]
                        )
                return carry

            lax.fori_loop(0, 4, push, 0)
            send_chunk(sb, rb, sb_sem, rb_sem, chunk, 1)

        for chunk in range(4):
            wait_chunk(rb, rb_sem, chunk)
        for ch in range(2):
            for par in range(2):
                lanes = pl.ds(128 * par, 128)
                conc = ra2[pl.ds(par, NT, stride=4), :]
                out_ref[ch, :, lanes] = rb2[pl.ds(2 * ch + par, NT, stride=4), :] + (1.0 - conc) * opn[ch, :, lanes]
        wait_bytes(sa, sa_sem)
        wait_bytes(sb, sb_sem)

    east = lax.rem(lo + 1, NLON)
    west = lax.rem(lo + NLON - 1, NLON)
    has_south = la > 0
    has_north = la < NLAT - 1

    def halo_copies(group, bufs):
        ss, sn, hs, hn, pk, pw, pe = bufs
        south, north = la - 1, la + 1
        low, high = pk.at[pl.ds(0, 8)], pk.at[pl.ds(120, 8)]
        below, above = pl.ds(0, 8), pl.ds(136, 8)
        plan = (
            (None, pk, pw.at[pl.ds(8, 128)], la, east),
            (None, pk, pe.at[pl.ds(8, 128)], la, west),
            (has_north, sn, hs, north, lo),
            (has_north, high, pw.at[below], north, east),
            (has_north, high, pe.at[below], north, west),
            (has_south, ss, hn, south, lo),
            (has_south, low, pw.at[above], south, east),
            (has_south, low, pe.at[above], south, west),
        )
        return [
            (
                cond,
                pltpu.make_async_remote_copy(
                    src_ref=src, dst_ref=dst, send_sem=h_send.at[8 * group + n], recv_sem=h_recv.at[8 * group + n],
                    device_id=(1, tla, tlo), device_id_type=MESH,
                ),
            )
            for n, (cond, src, dst, tla, tlo) in enumerate(plan)
        ]

    def under(cond, action):
        if cond is None:
            action()
        else:
            pl.when(cond)(action)

    def halo_start(group, bufs, source):
        ss, sn, hs, hn, pk, pw, pe = bufs
        count = ss.shape[0]
        for n in range(count):
            ss[n] = source(n)[pl.ds(0, 8), :]
            sn[n] = source(n)[pl.ds(120, 8), :]
        lane = lanes_of((8, 128))

        def pack(k, carry):
            rows = pl.ds(pl.multiple_of(8 * k, 8), 8)
            packed = jnp.zeros((8, 128), F32)
            for n in range(count):
                for par in range(2):
                    j = 2 * n + par
                    value = source(n)[rows, pl.ds(128 * par, 128)]
                    first = value if j == 0 else pltpu.roll(value, 4 * j, 1)
                    last = pltpu.roll(value, (4 * j - 60) % 128, 1)
                    packed = jnp.where((lane >= 4 * j) & (lane < 4 * j + 4), first, packed)
                    packed = jnp.where((lane >= 64 + 4 * j) & (lane < 68 + 4 * j), last, packed)
            pk[rows, :] = packed
            return carry

        lax.fori_loop(0, 16, pack, 0)
        for cond, copy in halo_copies(group, bufs):
            under(cond, copy.start)

    def halo_walls(bufs):
        ss, sn, hs, hn, pk, pw, pe = bufs
        zero = jnp.zeros((8, 128), F32)

        @pl.when(la == 0)
        def _():
            hs[...] = jnp.zeros(hs.shape, F32)
            pw[pl.ds(0, 8), :] = zero
            pe[pl.ds(0, 8), :] = zero

        @pl.when(la == NLAT - 1)
        def _():
            hn[...] = jnp.zeros(hn.shape, F32)
            pw[pl.ds(136, 8), :] = zero
            pe[pl.ds(136, 8), :] = zero

    def halo_finish(group, bufs, channels, source):
        ss, sn, hs, hn, pk, pw, pe = bufs
        copies = halo_copies(group, bufs)
        received = {2: has_south, 3: has_south, 4: has_south, 5: has_north, 6: has_north, 7: has_north}
        for n, (cond, copy) in enumerate(copies):
            under(received.get(n), copy.wait_recv)
        for n, channel in enumerate(channels):
            for par in range(2):
                lanes = pl.ds(128 * par, 128)
                x[2 * channel + par, pl.ds(8, 8), pl.ds(0, 128)] = hs[n, :, lanes]
                x[2 * channel + par, pl.ds(144, 8), pl.ds(0, 128)] = hn[n, :, lanes]
        lane = lanes_of((8, 128))

        def unpack(k, carry):
            rows = pl.ds(pl.multiple_of(8 * k, 8), 8)
            into = pl.ds(pl.multiple_of(8 * k + 8, 8), 8)
            from_west = pw[rows, :]
            from_east = pe[rows, :]
            for n, channel in enumerate(channels):
                for par in range(2):
                    j = 2 * n + par
                    right = from_east if j == 0 else pltpu.roll(from_east, 128 - 4 * j, 1)
                    left = pltpu.roll(from_west, (60 - 4 * j) % 128, 1)
                    x[2 * channel + par, into, pl.ds(128, 128)] = jnp.where(lane < 64, right, left)
            return carry

        lax.fori_loop(0, 18, unpack, 0)

        def main(k, carry):
            rows = pl.ds(pl.multiple_of(8 * k, 8), 8)
            into = pl.ds(pl.multiple_of(8 * k + TOP, 8), 8)
            for n, channel in enumerate(channels):
                for par in range(2):
                    x[2 * channel + par, into, pl.ds(0, 128)] = source(n)[rows, pl.ds(128 * par, 128)]
            return carry

        lax.fori_loop(0, 16, main, 0)

    def halo_sent(group, bufs):
        for cond, copy in halo_copies(group, bufs):
            under(cond, copy.wait_send)

    ice_bufs = (ss1, sn1, hs1, hn1, pk1, pw1, pe1)
    cur_bufs = (ss2, sn2, hs2, hn2, pk2, pw2, pe2)
    push_bufs = (ss3, sn3, hs3, hn3, pk3, pw3, pe3)

    @pl.when(comp == 1)
    def _():
        def greet(k, carry):
            t = lax.rem(me + k, NT)
            tla, tlo = t // NLON, lax.rem(t, NLON)

            @pl.when(k > 0)
            def _():
                pl.semaphore_signal(barrier, inc=1, device_id=(1, tla, tlo), device_id_type=MESH)

            pl.semaphore_signal(barrier, inc=1, device_id=(0, tla, tlo), device_id_type=MESH)
            return carry

        lax.fori_loop(0, NT, greet, 0)

        square = (NT, NT)
        diagonal = lax.broadcasted_iota(jnp.int32, square, 0) == lanes_of(square)
        covered = jnp.sum(jnp.where(diagonal, cov_ref[...].astype(F32), 0.0), axis=1, keepdims=True)
        act[...] = covered * (1 - land_ref[...]).astype(F32)
        halo_walls(ice_bufs)
        halo_walls(cur_bufs)
        halo_walls(push_bufs)

        pl.semaphore_wait(barrier, 2 * NT - 1)

        def tell(k, carry):
            t = lax.rem(me + k, NT)
            pltpu.make_async_remote_copy(
                src_ref=own_ref, dst_ref=ids.at[me], send_sem=id_send, recv_sem=id_recv,
                device_id=(1, t // NLON, lax.rem(t, NLON)), device_id_type=MESH,
            ).start()
            return carry

        lax.fori_loop(1, NT, tell, 0)
        ids[me] = own_ref[...]

        def ice_source(n):
            return f_ref.at[n] if n < 7 else act

        halo_start(0, ice_bufs, ice_source)

        wait_bytes(ids.at[pl.ds(0, NT - 1)], id_recv)
        every = ids.reshape(NT, NT)[...]
        local = jnp.where(lanes_of(square) == me, (every - NT * me).astype(F32), 0.0)
        local = jnp.sum(local, axis=1, keepdims=True)
        q = (local == lanes_of(square).astype(F32)).astype(F32)
        qmat[0] = q
        qmat[1] = q.T

        def to_slots(values):
            return jnp.dot(qmat[0], values, precision=HIGHEST, preferred_element_type=F32)

        def to_blocks(values):
            return jnp.dot(qmat[1], values, precision=HIGHEST, preferred_element_type=F32)

        a = act[...]
        for ch, value in enumerate((f_ref[3] * a, f_ref[2] * a)):
            moved = to_slots(value)
            for par in range(2):
                sa2[pl.ds(2 * ch + par, NT, stride=4), :] = moved[:, 128 * par : 128 * par + 128]
        for chunk in range(4):
            send_chunk(sa, ra, sa_sem, ra_sem, chunk, 0)

        halo_finish(0, ice_bufs, GROUP_ICE, ice_source)

        def prepare(k, carry):
            rows = pl.ds(pl.multiple_of(8 * k + 8, 8), 8)
            for par in range(2):
                conc = x[2 * DRAG + par, rows, :]
                active = x[2 * ACT + par, rows, :]
                x[2 * STR + par, rows, :] = x[2 * MASS + par, rows, :] * jnp.exp(2.0 * (conc - 1.0)) * active
                x[2 * DRAG + par, rows, :] = 1.5 * conc * active
            return carry

        lax.fori_loop(0, 18, prepare, 0)

        for chunk in range(4):
            wait_chunk(ra, ra_sem, chunk)
        for ch in range(2):
            for par in range(2):
                gat[ch, :, pl.ds(128 * par, 128)] = to_blocks(ra2[pl.ds(2 * ch + par, NT, stride=4), :])
        halo_start(1, cur_bufs, lambda n: gat.at[n])
        halo_finish(1, cur_bufs, GROUP_CUR, lambda n: gat.at[n])

        for chunk in range(4):
            wait_chunk(rb, rb_sem, chunk)
        for ch in range(2):
            for par in range(2):
                gat[2 + ch, :, pl.ds(128 * par, 128)] = to_blocks(rb2[pl.ds(2 * ch + par, NT, stride=4), :])
        halo_start(2, push_bufs, lambda n: gat.at[2 + n])
        halo_finish(2, push_bufs, GROUP_PUSH, lambda n: gat.at[2 + n])

        def get(channel, par, start):
            return x[2 * channel + par, pl.ds(start, 8), :]

        def east_of(value):
            return pltpu.roll(value, 255, 1)

        def west_of(value):
            return pltpu.roll(value, 1, 1)

        third = 1.0 / 1.5

        sub = lax.broadcasted_iota(jnp.int32, (8, 256), 0)

        def stress(k, carry):
            r = pl.multiple_of(8 * (18 - k), 8)
            u0, u1, v0, v1 = get(U, 0, r), get(U, 1, r), get(V, 0, r), get(V, 1, r)
            rolled = (pltpu.roll(u0, 7, 0), pltpu.roll(v0, 7, 0))
            u2, v2 = (jnp.where(sub == 7, after, here) for after, here in zip(carry, rolled))
            for par, u, v, un, vn in ((0, u0, v0, u1, v1), (1, u1, v1, u2, v2)):
                sxx = east_of(u) - u
                syy = vn - v
                shear = (un - u) + (east_of(v) - v)
                div = sxx + syy
                ten = sxx - syy
                strength = get(STR, par, r)
                visc = strength * lax.rsqrt(div * div + (ten * ten + shear * shear) * 0.25 + 0.25)
                rows = pl.ds(r, 8)
                x[2 * S1 + par, rows, :] = (get(S1, par, r) + 0.5 * (visc * div - strength)) * third
                x[2 * S2 + par, rows, :] = (get(S2, par, r) + 0.125 * visc * ten) * third
                x[2 * S12 + par, rows, :] = (get(S12, par, r) + 0.0625 * visc * shear) * third
            return rolled

        def momentum(k, carry):
            r = pl.multiple_of(8 * k + 8, 8)
            even, odd = (
                (0.5 * (get(S1, p, r) + get(S2, p, r)), 0.5 * (get(S1, p, r) - get(S2, p, r)), get(S12, p, r))
                for p in (0, 1)
            )
            rolled = (pltpu.roll(odd[1], 1, 0), pltpu.roll(odd[2], 1, 0))
            before = [None] + [jnp.where(sub == 0, below, here) for below, here in zip(carry, rolled)]
            for par, here, down in ((0, even, before), (1, odd, even)):
                xx, yy, s12 = here
                force_x = xx - west_of(xx) + (s12 - down[2])
                force_y = s12 - west_of(s12) + (yy - down[1])
                u, v, cx, cy = get(U, par, r), get(V, par, r), get(CX, par, r), get(CY, par, r)
                mass = get(MASS, par, r)
                dx = cx - u
                dy = cy - v
                drag = get(DRAG, par, r) * root(dx * dx + dy * dy + 0.1)
                scale = get(ACT, par, r) / (2.0 * jnp.maximum(mass, 0.5) + drag)
                mass2 = 2.0 * mass
                turn = 0.3 * mass
                rows = pl.ds(r, 8)
                x[2 * U + par, rows, :] = scale * (mass2 * u + force_x + get(PX, par, r) + drag * cx + turn * v)
                x[2 * V + par, rows, :] = scale * (mass2 * v + force_y + get(PY, par, r) + drag * cy - turn * u)
            return rolled

        zero = jnp.zeros((8, 256), F32)
        for repeat in range(NSUB):
            lax.fori_loop(0, 18, stress, (zero, zero))
            lax.fori_loop(0, 18, momentum, (zero, zero))

        inner = pl.ds(TOP, NT)
        main = pl.ds(0, 128)
        for par in range(2):
            u, v = x[2 * U + par, inner, main], x[2 * V + par, inner, main]
            dx = u - x[2 * CX + par, inner, main]
            dy = v - x[2 * CY + par, inner, main]
            factor = x[2 * DRAG + par, inner, main] * root(dx * dx + dy * dy + 0.1)
            lanes = pl.ds(128 * par, 128)
            sb2[pl.ds(par, NT, stride=4), :] = to_slots(factor * dx)
            sb2[pl.ds(2 + par, NT, stride=4), :] = to_slots(factor * dy)
            out_ref[0, :, lanes] = u
            out_ref[1, :, lanes] = v
        for chunk in range(4):
            send_chunk(sb, rb, sb_sem, rb_sem, chunk, 0)
        wait_bytes(ids.at[pl.ds(0, NT - 1)], id_send)
        for group, bufs in enumerate((ice_bufs, cur_bufs, push_bufs)):
            halo_sent(group, bufs)
        wait_bytes(sa, sa_sem)
        wait_bytes(sb, sb_sem)


def halo_scratch(count):
    return [
        pltpu.VMEM((count, 8, 256), F32),
        pltpu.VMEM((count, 8, 256), F32),
        pltpu.VMEM((count, 8, 256), F32),
        pltpu.VMEM((count, 8, 256), F32),
        pltpu.VMEM((128, 128), F32),
        pltpu.VMEM((144, 128), F32),
        pltpu.VMEM((144, 128), F32),
    ]


def per_device(fields, block_owner, ice_covered, land_mask):
    out = pl.pallas_call(
        kernel,
        out_shape=jax.ShapeDtypeStruct((2, NT, 256), F32),
        in_specs=[pl.BlockSpec(memory_space=pltpu.VMEM)] * 4,
        out_specs=pl.BlockSpec(memory_space=pltpu.VMEM),
        scratch_shapes=[
            pltpu.VMEM((NT, 1, NT), jnp.int32),
            *[pltpu.VMEM((4 * NT, 1, 128), F32)] * 4,
            pltpu.VMEM((26, ROWS, 256), F32),
            pltpu.VMEM((NT, 256), F32),
            pltpu.VMEM((4, NT, 256), F32),
            pltpu.VMEM((2, NT, 256), F32),
            pltpu.VMEM((2, NT, 256), F32),
            pltpu.VMEM((2, NT, NT), F32),
            *halo_scratch(8),
            *halo_scratch(2),
            *halo_scratch(2),
            pltpu.SemaphoreType.DMA,
            pltpu.SemaphoreType.DMA,
            pltpu.SemaphoreType.DMA,
            pltpu.SemaphoreType.DMA((4,)),
            pltpu.SemaphoreType.DMA,
            pltpu.SemaphoreType.DMA((4,)),
            pltpu.SemaphoreType.DMA((24,)),
            pltpu.SemaphoreType.DMA((24,)),
        ],
        compiler_params=pltpu.CompilerParams(
            collective_id=0, has_side_effects=True, vmem_limit_bytes=40 * 1024 * 1024
        ),
    )(fields[0], block_owner.reshape(1, NT), ice_covered.reshape(1, NT), land_mask)
    return out[None]


def solution(mesh):
    placed = (
        P("comp", None, ("lat", "lon"), None),
        P(("lat", "lon")),
        P(("lat", "lon")),
        P(("lat", "lon"), None),
    )
    return jax.shard_map(
        per_device,
        mesh=mesh,
        in_specs=placed,
        out_specs=P("comp", None, ("lat", "lon"), None),
        check_vma=False,
    )
```

```python
import functools

import jax
import jax.numpy as jnp
from jax import lax
from jax.experimental import pallas as pl
from jax.experimental.pallas import tpu as pltpu
from jax.sharding import PartitionSpec as P


NSUB = 4
NLAT = 8
NLON = 16
NT = NLAT * NLON
TOP = 16
ROWS = 160
MESH = pl.DeviceIdType.MESH
HIGHEST = lax.Precision.HIGHEST
F32 = jnp.float32

U, V, S1, S2, S12, STR, MASS, DRAG, ACT, CX, CY, PX, PY, SCALE = range(14)
RB = 16
GROUP_ICE = (U, V, MASS, DRAG, S1, S2, S12, ACT)
GROUP_CUR = (CX, CY)
GROUP_PUSH = (PX, PY)


def lanes_of(shape):
    return lax.broadcasted_iota(jnp.int32, shape, len(shape) - 1)


def root(x):
    return x * lax.rsqrt(x)


def kernel(
    f_hbm, own_hbm, cov_hbm, land_hbm, out_ref,
    f_ref, own_ref, cov_ref, land_ref, in_sem,
    ids, sa, ra, sb, rb, x, act, gat, opn, outb, qmat,
    ss1, sn1, hs1, hn1, pk1, pw1, pe1,
    ss2, sn2, hs2, hn2, pk2, pw2, pe2,
    ss3, sn3, hs3, hn3, pk3, pw3, pe3,
    id_send, id_recv, sa_sem, ra_sem, sb_sem, rb_sem, h_send, h_recv,
):
    comp = lax.axis_index("comp")
    la = lax.axis_index("lat")
    lo = lax.axis_index("lon")
    me = la * NLON + lo
    barrier = pltpu.get_barrier_semaphore()
    sa2, ra2, sb2, rb2 = (r.reshape(4 * NT, 128) for r in (sa, ra, sb, rb))

    loads = [
        pltpu.make_async_copy(src, dst, in_sem.at[n])
        for n, (src, dst) in enumerate(
            ((f_hbm, f_ref), (own_hbm, own_ref), (cov_hbm, cov_ref), (land_hbm, land_ref))
        )
    ]

    def greet(other):
        for tla in range(NLAT):
            for tlo in range(NLON):
                pl.semaphore_signal(barrier, inc=1, device_id=(other, tla, tlo), device_id_type=MESH)

    def target_core(chunk, level):
        core = lax.rem(lax.rem(la, 2) + chunk % 2, 2)
        return 2 * lax.rem(la // 2 + level, 4) + core

    def target_half(chunk):
        return 8 * lax.rem(lo // 8 + chunk // 2, 2)

    columns = [lax.rem(lax.rem(lo, 8) + j, 8) for j in range(8)]
    mine = pl.ds(4 * me, 4)

    def send_chunk(src, dst, send_sem, recv_sem, chunk, other):
        half = target_half(chunk)

        def body(level, carry):
            tla = target_core(chunk, level)
            base = tla * NLON + half
            for column in columns:
                pltpu.make_async_remote_copy(
                    src_ref=src.at[pl.ds(4 * (base + column), 4)],
                    dst_ref=dst.at[mine],
                    send_sem=send_sem,
                    recv_sem=recv_sem.at[chunk],
                    device_id=(other, tla, half + column),
                    device_id_type=MESH,
                ).start()
            return carry

        lax.fori_loop(0, 4, body, 0)

    def wait_bytes(ref, sem):
        pltpu.make_async_copy(ref, ref, sem).wait()

    def wait_chunk(dst, recv_sem, chunk):
        wait_bytes(dst.at[pl.ds(0, 128)], recv_sem.at[chunk])

    @pl.when(comp == 0)
    def _():
        loads[0].start()
        greet(1)
        loads[0].wait()
        for ch in range(2):
            for par in range(2):
                sa2[pl.ds(2 * ch + par, NT, stride=4), :] = f_ref[2 + ch, :, pl.ds(128 * par, 128)]
        pl.semaphore_wait(barrier, NT)
        for chunk in range(4):
            send_chunk(sa, ra, sa_sem, ra_sem, chunk, 1)

        def air(k, carry):
            rows = pl.ds(pl.multiple_of(8 * k, 8), 8)
            wx, wy, cx, cy, rho = (f_ref[i, rows, :] for i in (0, 1, 2, 3, 6))
            scale = rho * 0.1 * root(wx * wx + wy * wy + 1.0)
            outb[0, rows, :] = scale * wx
            outb[1, rows, :] = scale * wy
            rx = wx - cx
            ry = wy - cy
            speed = root(rx * rx + ry * ry + 1.0)
            scale = rho * (0.1 + 0.05 * speed) * speed
            opn[0, rows, :] = scale * rx
            opn[1, rows, :] = scale * ry
            return carry

        lax.fori_loop(0, 16, air, 0)

        for chunk in range(4):
            wait_chunk(ra, ra_sem, chunk)

            def push(level, carry):
                base = target_core(chunk, level) * NLON + target_half(chunk)
                rows = pl.ds(pl.multiple_of(base, 8), 8)
                for par in range(2):
                    lanes = pl.ds(128 * par, 128)
                    conc = ra2[pl.ds(4 * base + par, 8, stride=4), :]
                    mass = ra2[pl.ds(4 * base + 2 + par, 8, stride=4), :]
                    for ch in range(2):
                        sb2[pl.ds(4 * base + 2 * ch + par, 8, stride=4), :] = (
                            conc * outb[ch, rows, lanes] - mass * f_ref[4 + ch, rows, lanes]
                        )
                return carry

            lax.fori_loop(0, 4, push, 0)
            send_chunk(sb, rb, sb_sem, rb_sem, chunk, 1)

        for chunk in range(4):
            wait_chunk(rb, rb_sem, chunk)
        for ch in range(2):
            for par in range(2):
                lanes = pl.ds(128 * par, 128)
                conc = ra2[pl.ds(par, NT, stride=4), :]
                out_ref[ch, :, lanes] = rb2[pl.ds(2 * ch + par, NT, stride=4), :] + (1.0 - conc) * opn[ch, :, lanes]
        wait_bytes(sa, sa_sem)
        wait_bytes(sb, sb_sem)

    east = lax.rem(lo + 1, NLON)
    west = lax.rem(lo + NLON - 1, NLON)
    has_south = la > 0
    has_north = la < NLAT - 1

    def halo_copies(group, bufs):
        ss, sn, hs, hn, pk, pw, pe = bufs
        south, north = la - 1, la + 1
        low, high = pk.at[pl.ds(0, 8)], pk.at[pl.ds(120, 8)]
        below, above = pl.ds(0, 8), pl.ds(136, 8)
        plan = (
            (None, pk, pw.at[pl.ds(8, 128)], la, east),
            (None, pk, pe.at[pl.ds(8, 128)], la, west),
            (has_north, sn, hs, north, lo),
            (has_north, high, pw.at[below], north, east),
            (has_north, high, pe.at[below], north, west),
            (has_south, ss, hn, south, lo),
            (has_south, low, pw.at[above], south, east),
            (has_south, low, pe.at[above], south, west),
        )
        return [
            (
                cond,
                pltpu.make_async_remote_copy(
                    src_ref=src, dst_ref=dst, send_sem=h_send.at[8 * group + n], recv_sem=h_recv.at[8 * group + n],
                    device_id=(1, tla, tlo), device_id_type=MESH,
                ),
            )
            for n, (cond, src, dst, tla, tlo) in enumerate(plan)
        ]

    def under(cond, action):
        if cond is None:
            action()
        else:
            pl.when(cond)(action)

    def halo_start(group, bufs, source):
        ss, sn, hs, hn, pk, pw, pe = bufs
        count = ss.shape[0]
        for n in range(count):
            ss[n] = source(n)[pl.ds(0, 8), :]
            sn[n] = source(n)[pl.ds(120, 8), :]
        lane = lanes_of((NT, 128))
        packed = jnp.zeros((NT, 128), F32)
        for n in range(count):
            for par in range(2):
                j = 2 * n + par
                value = source(n)[:, pl.ds(128 * par, 128)]
                first = value if j == 0 else pltpu.roll(value, 4 * j, 1)
                last = pltpu.roll(value, (4 * j - 60) % 128, 1)
                packed = jnp.where((lane >= 4 * j) & (lane < 4 * j + 4), first, packed)
                packed = jnp.where((lane >= 64 + 4 * j) & (lane < 68 + 4 * j), last, packed)
        pk[...] = packed
        for cond, copy in halo_copies(group, bufs):
            under(cond, copy.start)

    def halo_walls(bufs):
        ss, sn, hs, hn, pk, pw, pe = bufs
        zero = jnp.zeros((8, 128), F32)

        @pl.when(la == 0)
        def _():
            hs[...] = jnp.zeros(hs.shape, F32)
            pw[pl.ds(0, 8), :] = zero
            pe[pl.ds(0, 8), :] = zero

        @pl.when(la == NLAT - 1)
        def _():
            hn[...] = jnp.zeros(hn.shape, F32)
            pw[pl.ds(136, 8), :] = zero
            pe[pl.ds(136, 8), :] = zero

    def halo_finish(group, bufs, channels, source, put):
        ss, sn, hs, hn, pk, pw, pe = bufs
        copies = halo_copies(group, bufs)
        received = {2: has_south, 3: has_south, 4: has_south, 5: has_north, 6: has_north, 7: has_north}
        for n, (cond, copy) in enumerate(copies):
            under(received.get(n), copy.wait_recv)
        lane = lanes_of((144, 128))
        from_west = pw[...]
        from_east = pe[...]
        for n, channel in enumerate(channels):
            for par in range(2):
                j = 2 * n + par
                lanes = pl.ds(128 * par, 128)
                right = from_east if j == 0 else pltpu.roll(from_east, 128 - 4 * j, 1)
                left = pltpu.roll(from_west, (60 - 4 * j) % 128, 1)
                put(channel, par, pl.ds(8, 144), pl.ds(128, 128), jnp.where(lane < 64, right, left))
                put(channel, par, pl.ds(8, 8), pl.ds(0, 128), hs[n, :, lanes])
                put(channel, par, pl.ds(144, 8), pl.ds(0, 128), hn[n, :, lanes])
                put(channel, par, pl.ds(TOP, NT), pl.ds(0, 128), source(n)[:, lanes])

    def put_x(channel, par, rows, lanes, value):
        x[2 * channel + par, rows, lanes] = value

    def put_push(channel, par, rows, lanes, value):
        put_x(channel, par, rows, lanes, value)
        velocity = 2 * (U if channel == PX else V) + par
        x[velocity, rows, lanes] += x[2 * SCALE + par, rows, lanes] * value

    def halo_sent(group, bufs):
        for cond, copy in halo_copies(group, bufs):
            under(cond, copy.wait_send)

    ice_bufs = (ss1, sn1, hs1, hn1, pk1, pw1, pe1)
    cur_bufs = (ss2, sn2, hs2, hn2, pk2, pw2, pe2)
    push_bufs = (ss3, sn3, hs3, hn3, pk3, pw3, pe3)

    @pl.when(comp == 1)
    def _():
        for load in loads:
            load.start()
        greet(0)
        greet(1)
        for load in loads:
            load.wait()
        square = (NT, NT)
        diagonal = lax.broadcasted_iota(jnp.int32, square, 0) == lanes_of(square)
        covered = jnp.sum(jnp.where(diagonal, cov_ref[...].astype(F32), 0.0), axis=1, keepdims=True)
        act[...] = covered * (1 - land_ref[...]).astype(F32)
        halo_walls(ice_bufs)
        halo_walls(cur_bufs)
        halo_walls(push_bufs)

        pl.semaphore_wait(barrier, 2 * NT)

        others = [lax.rem(lo + j, NLON) for j in range(NLON)]

        def tell_one(tla, tlo):
            pltpu.make_async_remote_copy(
                src_ref=own_ref, dst_ref=ids.at[me], send_sem=id_send, recv_sem=id_recv,
                device_id=(1, tla, tlo), device_id_type=MESH,
            ).start()

        for tlo in others[1:]:
            tell_one(la, tlo)

        def tell(k, carry):
            tla = lax.rem(la + k, NLAT)
            for tlo in others:
                tell_one(tla, tlo)
            return carry

        lax.fori_loop(1, NLAT, tell, 0)
        ids[me] = own_ref[...]

        def ice_source(n):
            return f_ref.at[n] if n < 7 else act

        halo_start(0, ice_bufs, ice_source)

        wait_bytes(ids.at[pl.ds(0, NT - 1)], id_recv)
        every = ids.reshape(NT, NT)[...]
        local = jnp.where(lanes_of(square) == me, (every - NT * me).astype(F32), 0.0)
        local = jnp.sum(local, axis=1, keepdims=True)
        q = (local == lanes_of(square).astype(F32)).astype(F32)
        qmat[0] = q
        qmat[1] = q.T

        def to_slots(values):
            return jnp.dot(qmat[0], values, precision=HIGHEST, preferred_element_type=F32)

        def to_blocks(values):
            return jnp.dot(qmat[1], values, precision=HIGHEST, preferred_element_type=F32)

        a = act[...]
        for ch, value in enumerate((f_ref[3] * a, f_ref[2] * a)):
            moved = to_slots(value)
            for par in range(2):
                sa2[pl.ds(2 * ch + par, NT, stride=4), :] = moved[:, 128 * par : 128 * par + 128]
        for chunk in range(4):
            send_chunk(sa, ra, sa_sem, ra_sem, chunk, 0)

        halo_finish(0, ice_bufs, GROUP_ICE, ice_source, put_x)

        def prepare(k, carry):
            rows = pl.ds(pl.multiple_of(8 * k + 8, 8), 8)
            for par in range(2):
                conc = x[2 * DRAG + par, rows, :]
                active = x[2 * ACT + par, rows, :]
                x[2 * STR + par, rows, :] = x[2 * MASS + par, rows, :] * jnp.exp(2.0 * (conc - 1.0)) * active
                x[2 * DRAG + par, rows, :] = 1.5 * conc * active
            return carry

        lax.fori_loop(0, 18, prepare, 0)

        for chunk in range(4):
            wait_chunk(ra, ra_sem, chunk)
        for ch in range(2):
            for par in range(2):
                gat[ch, :, pl.ds(128 * par, 128)] = to_blocks(ra2[pl.ds(2 * ch + par, NT, stride=4), :])
        halo_start(1, cur_bufs, lambda n: gat.at[n])
        halo_finish(1, cur_bufs, GROUP_CUR, lambda n: gat.at[n], put_x)

        def get(channel, par, start):
            return x[2 * channel + par, pl.ds(start, RB), :]

        def east_of(value):
            return pltpu.roll(value, 255, 1)

        def west_of(value):
            return pltpu.roll(value, 1, 1)

        third = 1.0 / 1.5
        sub = lax.broadcasted_iota(jnp.int32, (RB, 256), 0)
        zero = jnp.zeros((RB, 256), F32)
        steps = 144 // RB

        def stress(k, carry):
            r = pl.multiple_of(RB * (steps - 1 - k) + 8, 8)
            u0, u1, v0, v1 = get(U, 0, r), get(U, 1, r), get(V, 0, r), get(V, 1, r)
            rolled = (pltpu.roll(u0, RB - 1, 0), pltpu.roll(v0, RB - 1, 0))
            u2, v2 = (jnp.where(sub == RB - 1, after, here) for after, here in zip(carry, rolled))
            for par, u, v, un, vn in ((0, u0, v0, u1, v1), (1, u1, v1, u2, v2)):
                sxx = east_of(u) - u
                syy = vn - v
                shear = (un - u) + (east_of(v) - v)
                div = sxx + syy
                ten = sxx - syy
                strength = get(STR, par, r)
                visc = strength * lax.rsqrt(div * div + (ten * ten + shear * shear) * 0.25 + 0.25)
                rows = pl.ds(r, RB)
                x[2 * S1 + par, rows, :] = (get(S1, par, r) + 0.5 * (visc * div - strength)) * third
                x[2 * S2 + par, rows, :] = (get(S2, par, r) + 0.125 * visc * ten) * third
                x[2 * S12 + par, rows, :] = (get(S12, par, r) + 0.0625 * visc * shear) * third
            return rolled

        def momentum(first, k, carry):
            r = pl.multiple_of(RB * k + 8, 8)
            even, odd = (
                (0.5 * (get(S1, p, r) + get(S2, p, r)), 0.5 * (get(S1, p, r) - get(S2, p, r)), get(S12, p, r))
                for p in (0, 1)
            )
            rolled = (pltpu.roll(odd[1], 1, 0), pltpu.roll(odd[2], 1, 0))
            before = [None] + [jnp.where(sub == 0, below, here) for below, here in zip(carry, rolled)]
            for par, here, down in ((0, even, before), (1, odd, even)):
                xx, yy, s12 = here
                force_x = xx - west_of(xx) + (s12 - down[2])
                force_y = s12 - west_of(s12) + (yy - down[1])
                u, v, cx, cy = get(U, par, r), get(V, par, r), get(CX, par, r), get(CY, par, r)
                mass = get(MASS, par, r)
                dx = cx - u
                dy = cy - v
                drag = get(DRAG, par, r) * root(dx * dx + dy * dy + 0.1)
                scale = get(ACT, par, r) / (2.0 * jnp.maximum(mass, 0.5) + drag)
                mass2 = 2.0 * mass
                turn = 0.3 * mass
                rows = pl.ds(r, RB)
                if first:
                    x[2 * SCALE + par, rows, :] = scale
                else:
                    force_x = force_x + get(PX, par, r)
                    force_y = force_y + get(PY, par, r)
                x[2 * U + par, rows, :] = scale * (mass2 * u + force_x + drag * cx + turn * v)
                x[2 * V + par, rows, :] = scale * (mass2 * v + force_y + drag * cy - turn * u)
            return rolled

        def subcycle(first):
            lax.fori_loop(0, steps, stress, (zero, zero))
            lax.fori_loop(0, steps, functools.partial(momentum, first), (zero, zero))

        subcycle(True)

        for chunk in range(4):
            wait_chunk(rb, rb_sem, chunk)
        for ch in range(2):
            for par in range(2):
                gat[2 + ch, :, pl.ds(128 * par, 128)] = to_blocks(rb2[pl.ds(2 * ch + par, NT, stride=4), :])
        halo_start(2, push_bufs, lambda n: gat.at[2 + n])
        halo_finish(2, push_bufs, GROUP_PUSH, lambda n: gat.at[2 + n], put_push)

        for repeat in range(NSUB - 1):
            subcycle(False)

        inner = pl.ds(TOP, NT)
        main = pl.ds(0, 128)
        for par in range(2):
            u, v = x[2 * U + par, inner, main], x[2 * V + par, inner, main]
            dx = u - x[2 * CX + par, inner, main]
            dy = v - x[2 * CY + par, inner, main]
            factor = x[2 * DRAG + par, inner, main] * root(dx * dx + dy * dy + 0.1)
            lanes = pl.ds(128 * par, 128)
            sb2[pl.ds(par, NT, stride=4), :] = to_slots(factor * dx)
            sb2[pl.ds(2 + par, NT, stride=4), :] = to_slots(factor * dy)
            out_ref[0, :, lanes] = u
            out_ref[1, :, lanes] = v
        for chunk in range(4):
            send_chunk(sb, rb, sb_sem, rb_sem, chunk, 0)
        wait_bytes(ids.at[pl.ds(0, NT - 1)], id_send)
        for group, bufs in enumerate((ice_bufs, cur_bufs, push_bufs)):
            halo_sent(group, bufs)
        wait_bytes(sa, sa_sem)
        wait_bytes(sb, sb_sem)


def halo_scratch(count):
    return [
        pltpu.VMEM((count, 8, 256), F32),
        pltpu.VMEM((count, 8, 256), F32),
        pltpu.VMEM((count, 8, 256), F32),
        pltpu.VMEM((count, 8, 256), F32),
        pltpu.VMEM((128, 128), F32),
        pltpu.VMEM((144, 128), F32),
        pltpu.VMEM((144, 128), F32),
    ]


def per_device(fields, block_owner, ice_covered, land_mask):
    out = pl.pallas_call(
        kernel,
        out_shape=jax.ShapeDtypeStruct((2, NT, 256), F32),
        in_specs=[pl.BlockSpec(memory_space=pltpu.HBM)] * 4,
        out_specs=pl.BlockSpec(memory_space=pltpu.VMEM),
        scratch_shapes=[
            pltpu.VMEM((7, NT, 256), F32),
            pltpu.VMEM((1, NT), jnp.int32),
            pltpu.VMEM((1, NT), jnp.int32),
            pltpu.VMEM((NT, 256), jnp.int32),
            pltpu.SemaphoreType.DMA((4,)),
            pltpu.VMEM((NT, 1, NT), jnp.int32),
            *[pltpu.VMEM((4 * NT, 1, 128), F32)] * 4,
            pltpu.VMEM((28, ROWS, 256), F32),
            pltpu.VMEM((NT, 256), F32),
            pltpu.VMEM((4, NT, 256), F32),
            pltpu.VMEM((2, NT, 256), F32),
            pltpu.VMEM((2, NT, 256), F32),
            pltpu.VMEM((2, NT, NT), F32),
            *halo_scratch(8),
            *halo_scratch(2),
            *halo_scratch(2),
            pltpu.SemaphoreType.DMA,
            pltpu.SemaphoreType.DMA,
            pltpu.SemaphoreType.DMA,
            pltpu.SemaphoreType.DMA((4,)),
            pltpu.SemaphoreType.DMA,
            pltpu.SemaphoreType.DMA((4,)),
            pltpu.SemaphoreType.DMA((24,)),
            pltpu.SemaphoreType.DMA((24,)),
        ],
        compiler_params=pltpu.CompilerParams(
            collective_id=0, has_side_effects=True, vmem_limit_bytes=60 * 1024 * 1024
        ),
    )(fields[0], block_owner.reshape(1, NT), ice_covered.reshape(1, NT), land_mask)
    return out[None]


def solution(mesh):
    placed = (
        P("comp", None, ("lat", "lon"), None),
        P(("lat", "lon")),
        P(("lat", "lon")),
        P(("lat", "lon"), None),
    )
    return jax.shard_map(
        per_device,
        mesh=mesh,
        in_specs=placed,
        out_specs=P("comp", None, ("lat", "lon"), None),
        check_vma=False,
    )
```

```python
import functools

import jax
import jax.numpy as jnp
from jax import lax
from jax.experimental import pallas as pl
from jax.experimental.pallas import tpu as pltpu
from jax.sharding import PartitionSpec as P


NSUB = 4
NLAT = 8
NLON = 16
NT = NLAT * NLON
TOP = 16
ROWS = 160
MESH = pl.DeviceIdType.MESH
HIGHEST = lax.Precision.HIGHEST
F32 = jnp.float32

U, V, S1, S2, S12, STR, MASS, DRAG, ACT, CX, CY, PX, PY, SCALE = range(14)
RB = 16
GROUP_ICE = (U, V, MASS, DRAG, S1, S2, S12, ACT)
GROUP_CUR = (CX, CY)
GROUP_PUSH = (PX, PY)


def lanes_of(shape):
    return lax.broadcasted_iota(jnp.int32, shape, len(shape) - 1)


def root(x):
    return x * lax.rsqrt(x)


def kernel(
    f_hbm, own_hbm, cov_hbm, land_hbm, out_ref,
    f_ref, own_ref, cov_ref, land_ref, in_sem,
    ids, sa, ra, sb, rb, sd, rd, x, act, gat, opn, outb, qmat,
    ss1, sn1, hs1, hn1, se1, sw1, pw1, pe1,
    ss2, sn2, hs2, hn2, se2, sw2, pw2, pe2,
    ss3, sn3, hs3, hn3, se3, sw3, pw3, pe3,
    id_send, id_recv, sa_sem, ra_sem, sb_sem, rb_sem, sd_sem, rd_sem, h_send, h_recv,
):
    comp = lax.axis_index("comp")
    la = lax.axis_index("lat")
    lo = lax.axis_index("lon")
    me = la * NLON + lo
    barrier = pltpu.get_barrier_semaphore()
    sa2, ra2, sb2, rb2 = (r.reshape(4 * NT, 128) for r in (sa, ra, sb, rb))
    sd2, rd2 = (r.reshape(8 * NT, 128) for r in (sd, rd))

    loads = [
        pltpu.make_async_copy(src, dst, in_sem.at[n])
        for n, (src, dst) in enumerate(
            ((f_hbm, f_ref), (own_hbm, own_ref), (cov_hbm, cov_ref), (land_hbm, land_ref))
        )
    ]

    def greet(other):
        for tla in range(NLAT):
            for tlo in range(NLON):
                pl.semaphore_signal(barrier, inc=1, device_id=(other, tla, tlo), device_id_type=MESH)

    others = [lax.rem(lo + j, NLON) for j in range(NLON)]

    def target_lat(chunk, k, other):
        offset = 2 * chunk + k
        return lax.rem(la + (NLAT - offset if other == 1 else offset), NLAT)

    def send_chunk(src, dst, send_sem, recv_sem, chunk, other, stride=4, rows=4):
        def body(k, carry):
            tla = target_lat(chunk, k, other)
            for tlo in others:
                pltpu.make_async_remote_copy(
                    src_ref=src.at[pl.ds(stride * (tla * NLON + tlo), rows)],
                    dst_ref=dst.at[pl.ds(stride * me, rows)],
                    send_sem=send_sem,
                    recv_sem=recv_sem.at[chunk],
                    device_id=(other, tla, tlo),
                    device_id_type=MESH,
                ).start()
            return carry

        lax.fori_loop(0, 2, body, 0)

    def wait_bytes(ref, sem):
        pltpu.make_async_copy(ref, ref, sem).wait()

    def wait_chunk(dst, recv_sem, chunk, rows=4):
        wait_bytes(dst.at[pl.ds(0, 32 * rows)], recv_sem.at[chunk])

    def rows_of(chunk, level):
        return pl.multiple_of(target_lat(chunk, level // 2, 1) * NLON + 8 * lax.rem(level, 2), 8)

    @pl.when(comp == 0)
    def _():
        loads[0].start()
        greet(1)
        loads[0].wait()
        for ch in range(2):
            for par in range(2):
                sa2[pl.ds(2 * ch + par, NT, stride=4), :] = f_ref[2 + ch, :, pl.ds(128 * par, 128)]
        def air(k, carry):
            rows = pl.ds(pl.multiple_of(8 * k, 8), 8)
            wx, wy, cx, cy, rho = (f_ref[i, rows, :] for i in (0, 1, 2, 3, 6))
            scale = rho * 0.1 * root(wx * wx + wy * wy + 1.0)
            outb[0, rows, :] = scale * wx
            outb[1, rows, :] = scale * wy
            rx = wx - cx
            ry = wy - cy
            speed = root(rx * rx + ry * ry + 1.0)
            scale = rho * (0.1 + 0.05 * speed) * speed
            opn[0, rows, :] = scale * rx
            opn[1, rows, :] = scale * ry
            return carry

        lax.fori_loop(0, 16, air, 0)


        def direct(level, carry):
            base = rows_of(0, level)
            for par in range(2):
                lanes = pl.ds(128 * par, 128)
                for ch in range(2):
                    sd2[pl.ds(8 * base + 2 * ch + par, 8, stride=8), :] = outb[ch, pl.ds(base, 8), lanes]
                    sd2[pl.ds(8 * base + 4 + 2 * ch + par, 8, stride=8), :] = f_ref[4 + ch, pl.ds(base, 8), lanes]
            return carry

        lax.fori_loop(0, 4, direct, 0)
        pl.semaphore_wait(barrier, NT)
        for chunk in range(4):
            send_chunk(sa, ra, sa_sem, ra_sem, chunk, 1)
        send_chunk(sd, rd, sd_sem, rd_sem, 0, 1, 8, 8)

        for chunk in range(1, 4):
            wait_chunk(ra, ra_sem, chunk)

            def push(level, carry):
                base = rows_of(chunk, level)
                rows = pl.ds(base, 8)
                for par in range(2):
                    lanes = pl.ds(128 * par, 128)
                    conc = ra2[pl.ds(4 * base + par, 8, stride=4), :]
                    mass = ra2[pl.ds(4 * base + 2 + par, 8, stride=4), :]
                    for ch in range(2):
                        sb2[pl.ds(4 * base + 2 * ch + par, 8, stride=4), :] = (
                            conc * outb[ch, rows, lanes] - mass * f_ref[4 + ch, rows, lanes]
                        )
                return carry

            lax.fori_loop(0, 4, push, 0)
            send_chunk(sb, rb, sb_sem, rb_sem, chunk, 1)

        for chunk in range(4):
            wait_chunk(rb, rb_sem, chunk)
        wait_chunk(ra, ra_sem, 0, 2)
        for ch in range(2):
            for par in range(2):
                lanes = pl.ds(128 * par, 128)
                conc = ra2[pl.ds(par, NT, stride=4), :]
                out_ref[ch, :, lanes] = rb2[pl.ds(2 * ch + par, NT, stride=4), :] + (1.0 - conc) * opn[ch, :, lanes]
        wait_bytes(sa, sa_sem)
        wait_bytes(sb.at[pl.ds(0, 384)], sb_sem)
        wait_bytes(sd.at[pl.ds(0, 256)], sd_sem)

    east = lax.rem(lo + 1, NLON)
    west = lax.rem(lo + NLON - 1, NLON)
    has_south = la > 0
    has_north = la < NLAT - 1

    def halo_copies(group, bufs):
        ss, sn, hs, hn, se, sw, pw, pe = bufs
        size = se.shape[0]
        south, north = la - 1, la + 1
        first, last = pl.ds(0, 8), pl.ds(size - 8, 8)
        below, middle, above = pl.ds(0, 8), pl.ds(8, size), pl.ds(8 + size, 8)
        plan = (
            (None, se, pw.at[middle], la, east),
            (None, sw, pe.at[middle], la, west),
            (has_north, sn, hs, north, lo),
            (has_north, se.at[last], pw.at[below], north, east),
            (has_north, sw.at[last], pe.at[below], north, west),
            (has_south, ss, hn, south, lo),
            (has_south, se.at[first], pw.at[above], south, east),
            (has_south, sw.at[first], pe.at[above], south, west),
        )
        return [
            (
                cond,
                pltpu.make_async_remote_copy(
                    src_ref=src, dst_ref=dst, send_sem=h_send.at[8 * group + n], recv_sem=h_recv.at[8 * group + n],
                    device_id=(1, tla, tlo), device_id_type=MESH,
                ),
            )
            for n, (cond, src, dst, tla, tlo) in enumerate(plan)
        ]

    def under(cond, action):
        if cond is None:
            action()
        else:
            pl.when(cond)(action)

    def halo_start(group, bufs, source):
        ss, sn, hs, hn, se, sw, pw, pe = bufs
        count, size = ss.shape[0], se.shape[0]
        for n in range(count):
            ss[n] = source(n)[pl.ds(0, 2), :]
            sn[n] = source(n)[pl.ds(126, 2), :]
        lane = lanes_of((size, 128))
        to_east = jnp.zeros((size, 128), F32)
        to_west = to_east
        for g in range(NT // size):
            for n in range(count):
                for par in range(2):
                    at = 8 * count * g + 8 * n + 4 * par
                    value = source(n)[pl.ds(size * g, size), pl.ds(128 * par, 128)]
                    here = (lane >= at) & (lane < at + 4)
                    to_west = jnp.where(here, pltpu.roll(value, at, 1) if at else value, to_west)
                    to_east = jnp.where(here, pltpu.roll(value, (at - 124) % 128, 1) if at != 124 else value, to_east)
        se[...] = to_east
        sw[...] = to_west
        for cond, copy in halo_copies(group, bufs):
            under(cond, copy.start)

    def halo_walls(bufs):
        ss, sn, hs, hn, se, sw, pw, pe = bufs
        size = se.shape[0]
        zero = jnp.zeros((8, 128), F32)

        @pl.when(la == 0)
        def _():
            hs[...] = jnp.zeros(hs.shape, F32)
            pw[pl.ds(0, 8), :] = zero
            pe[pl.ds(0, 8), :] = zero

        @pl.when(la == NLAT - 1)
        def _():
            hn[...] = jnp.zeros(hn.shape, F32)
            pw[pl.ds(8 + size, 8), :] = zero
            pe[pl.ds(8 + size, 8), :] = zero

    def halo_finish(group, bufs, channels, source, put):
        ss, sn, hs, hn, se, sw, pw, pe = bufs
        count, size = ss.shape[0], se.shape[0]
        copies = halo_copies(group, bufs)
        received = {2: has_south, 3: has_south, 4: has_south, 5: has_north, 6: has_north, 7: has_north}
        for n, (cond, copy) in enumerate(copies):
            under(received.get(n), copy.wait_recv)
        groups = NT // size
        parts = [(TOP + size * g, size, 8, g) for g in range(groups)]
        parts += [(8, 8, 0, groups - 1), (TOP + NT, 8, 8 + size, 0)]
        for start, rows, at, g in parts:
            from_west = pw[pl.ds(at, rows), :]
            from_east = pe[pl.ds(at, rows), :]
            lane = lanes_of((rows, 128))
            for n, channel in enumerate(channels):
                for par in range(2):
                    j = 8 * count * g + 8 * n + 4 * par
                    right = pltpu.roll(from_east, 128 - j, 1) if j else from_east
                    left = pltpu.roll(from_west, 124 - j, 1) if j != 124 else from_west
                    put(channel, par, pl.ds(start, rows), pl.ds(128, 128), jnp.where(lane < 64, right, left))
        for n, channel in enumerate(channels):
            for par in range(2):
                lanes = pl.ds(128 * par, 128)
                put(channel, par, pl.ds(TOP - 2, 2), pl.ds(0, 128), hs[n, :, lanes])
                put(channel, par, pl.ds(TOP + NT, 2), pl.ds(0, 128), hn[n, :, lanes])
                put(channel, par, pl.ds(TOP, NT), pl.ds(0, 128), source(n)[:, lanes])

    def put_x(channel, par, rows, lanes, value):
        x[2 * channel + par, rows, lanes] = value

    def put_push(channel, par, rows, lanes, value):
        put_x(channel, par, rows, lanes, value)
        velocity = 2 * (U if channel == PX else V) + par
        x[velocity, rows, lanes] += x[2 * SCALE + par, rows, lanes] * value

    def halo_sent(group, bufs):
        for cond, copy in halo_copies(group, bufs):
            under(cond, copy.wait_send)

    ice_bufs = (ss1, sn1, hs1, hn1, se1, sw1, pw1, pe1)
    cur_bufs = (ss2, sn2, hs2, hn2, se2, sw2, pw2, pe2)
    push_bufs = (ss3, sn3, hs3, hn3, se3, sw3, pw3, pe3)

    @pl.when(comp == 1)
    def _():
        for load in loads:
            load.start()
        rb[...] = jnp.zeros(rb.shape, F32)
        rd[...] = jnp.zeros(rd.shape, F32)
        greet(0)
        greet(1)
        for load in loads:
            load.wait()
        square = (NT, NT)
        diagonal = lax.broadcasted_iota(jnp.int32, square, 0) == lanes_of(square)
        covered = jnp.sum(jnp.where(diagonal, cov_ref[...].astype(F32), 0.0), axis=1, keepdims=True)
        act[...] = covered * (1 - land_ref[...]).astype(F32)
        halo_walls(ice_bufs)
        halo_walls(cur_bufs)
        halo_walls(push_bufs)

        pl.semaphore_wait(barrier, 2 * NT)

        def tell_one(tla, tlo):
            pltpu.make_async_remote_copy(
                src_ref=own_ref, dst_ref=ids.at[me], send_sem=id_send, recv_sem=id_recv,
                device_id=(1, tla, tlo), device_id_type=MESH,
            ).start()

        for tlo in others[1:]:
            tell_one(la, tlo)

        def tell(k, carry):
            tla = lax.rem(la + k, NLAT)
            for tlo in others:
                tell_one(tla, tlo)
            return carry

        lax.fori_loop(1, NLAT, tell, 0)
        ids[me] = own_ref[...]

        def ice_source(n):
            return f_ref.at[n] if n < 7 else act

        halo_start(0, ice_bufs, ice_source)

        wait_bytes(ids.at[pl.ds(0, NT - 1)], id_recv)
        every = ids.reshape(NT, NT)[...]
        local = jnp.where(lanes_of(square) == me, (every - NT * me).astype(F32), 0.0)
        local = jnp.sum(local, axis=1, keepdims=True)
        q = (local == lanes_of(square).astype(F32)).astype(F32)
        qmat[0] = q
        qmat[1] = q.T

        def to_slots(values):
            return jnp.dot(qmat[0], values, precision=HIGHEST, preferred_element_type=F32)

        def to_blocks(values):
            return jnp.dot(qmat[1], values, precision=HIGHEST, preferred_element_type=F32)

        a = act[...]
        for ch, value in enumerate((f_ref[3] * a, f_ref[2] * a)):
            moved = to_slots(value)
            for par in range(2):
                sa2[pl.ds(2 * ch + par, NT, stride=4), :] = moved[:, 128 * par : 128 * par + 128]
        for chunk in range(1, 4):
            send_chunk(sa, ra, sa_sem, ra_sem, chunk, 0)
        send_chunk(sa, ra, sa_sem, ra_sem, 0, 0, 4, 2)
        halo_finish(0, ice_bufs, GROUP_ICE, ice_source, put_x)

        def prepare(k, carry):
            rows = pl.ds(pl.multiple_of(8 * k + 8, 8), 8)
            for par in range(2):
                conc = x[2 * DRAG + par, rows, :]
                active = x[2 * ACT + par, rows, :]
                x[2 * STR + par, rows, :] = x[2 * MASS + par, rows, :] * jnp.exp(2.0 * (conc - 1.0)) * active
                x[2 * DRAG + par, rows, :] = 1.5 * conc * active
            return carry

        lax.fori_loop(0, 18, prepare, 0)

        for chunk in range(4):
            wait_chunk(ra, ra_sem, chunk)
        for ch in range(2):
            for par in range(2):
                gat[ch, :, pl.ds(128 * par, 128)] = to_blocks(ra2[pl.ds(2 * ch + par, NT, stride=4), :])
        halo_start(1, cur_bufs, lambda n: gat.at[n])
        halo_finish(1, cur_bufs, GROUP_CUR, lambda n: gat.at[n], put_x)

        def get(channel, par, start):
            return x[2 * channel + par, pl.ds(start, RB), :]

        def east_of(value):
            return pltpu.roll(value, 255, 1)

        def west_of(value):
            return pltpu.roll(value, 1, 1)

        third = 1.0 / 1.5
        sub = lax.broadcasted_iota(jnp.int32, (RB, 256), 0)
        zero = jnp.zeros((RB, 256), F32)
        steps = 144 // RB

        def stress(k, carry):
            r = pl.multiple_of(RB * (steps - 1 - k) + 8, 8)
            u0, u1, v0, v1 = get(U, 0, r), get(U, 1, r), get(V, 0, r), get(V, 1, r)
            rolled = (pltpu.roll(u0, RB - 1, 0), pltpu.roll(v0, RB - 1, 0))
            u2, v2 = (jnp.where(sub == RB - 1, after, here) for after, here in zip(carry, rolled))
            for par, u, v, un, vn in ((0, u0, v0, u1, v1), (1, u1, v1, u2, v2)):
                sxx = east_of(u) - u
                syy = vn - v
                shear = (un - u) + (east_of(v) - v)
                div = sxx + syy
                ten = sxx - syy
                strength = get(STR, par, r)
                visc = strength * lax.rsqrt(div * div + (ten * ten + shear * shear) * 0.25 + 0.25)
                rows = pl.ds(r, RB)
                x[2 * S1 + par, rows, :] = (get(S1, par, r) + 0.5 * (visc * div - strength)) * third
                x[2 * S2 + par, rows, :] = (get(S2, par, r) + 0.125 * visc * ten) * third
                x[2 * S12 + par, rows, :] = (get(S12, par, r) + 0.0625 * visc * shear) * third
            return rolled

        def momentum(first, k, carry):
            r = pl.multiple_of(RB * k + 8, 8)
            even, odd = (
                (0.5 * (get(S1, p, r) + get(S2, p, r)), 0.5 * (get(S1, p, r) - get(S2, p, r)), get(S12, p, r))
                for p in (0, 1)
            )
            rolled = (pltpu.roll(odd[1], 1, 0), pltpu.roll(odd[2], 1, 0))
            before = [None] + [jnp.where(sub == 0, below, here) for below, here in zip(carry, rolled)]
            for par, here, down in ((0, even, before), (1, odd, even)):
                xx, yy, s12 = here
                force_x = xx - west_of(xx) + (s12 - down[2])
                force_y = s12 - west_of(s12) + (yy - down[1])
                u, v, cx, cy = get(U, par, r), get(V, par, r), get(CX, par, r), get(CY, par, r)
                mass = get(MASS, par, r)
                dx = cx - u
                dy = cy - v
                drag = get(DRAG, par, r) * root(dx * dx + dy * dy + 0.1)
                scale = get(ACT, par, r) / (2.0 * jnp.maximum(mass, 0.5) + drag)
                mass2 = 2.0 * mass
                turn = 0.3 * mass
                rows = pl.ds(r, RB)
                if first:
                    x[2 * SCALE + par, rows, :] = scale
                else:
                    force_x = force_x + get(PX, par, r)
                    force_y = force_y + get(PY, par, r)
                x[2 * U + par, rows, :] = scale * (mass2 * u + force_x + drag * cx + turn * v)
                x[2 * V + par, rows, :] = scale * (mass2 * v + force_y + drag * cy - turn * u)
            return rolled

        def subcycle(first):
            lax.fori_loop(0, steps, stress, (zero, zero))
            lax.fori_loop(0, steps, functools.partial(momentum, first), (zero, zero))

        subcycle(True)

        wait_chunk(rd, rd_sem, 0, 8)
        for par in range(2):
            lanes = pl.ds(128 * par, 128)
            for ch in range(2):
                stress_of_air = to_blocks(rd2[pl.ds(2 * ch + par, NT, stride=8), :])
                tilt = to_blocks(rd2[pl.ds(4 + 2 * ch + par, NT, stride=8), :])
                gat[2 + ch, :, lanes] = act[:, lanes] * (f_ref[3, :, lanes] * stress_of_air - f_ref[2, :, lanes] * tilt)
        for chunk in range(1, 4):
            wait_chunk(rb, rb_sem, chunk)
        for ch in range(2):
            for par in range(2):
                gat[2 + ch, :, pl.ds(128 * par, 128)] += to_blocks(rb2[pl.ds(2 * ch + par, NT, stride=4), :])
        halo_start(2, push_bufs, lambda n: gat.at[2 + n])
        halo_finish(2, push_bufs, GROUP_PUSH, lambda n: gat.at[2 + n], put_push)

        for repeat in range(NSUB - 1):
            subcycle(False)

        inner = pl.ds(TOP, NT)
        main = pl.ds(0, 128)
        for par in range(2):
            u, v = x[2 * U + par, inner, main], x[2 * V + par, inner, main]
            dx = u - x[2 * CX + par, inner, main]
            dy = v - x[2 * CY + par, inner, main]
            factor = x[2 * DRAG + par, inner, main] * root(dx * dx + dy * dy + 0.1)
            lanes = pl.ds(128 * par, 128)
            sb2[pl.ds(par, NT, stride=4), :] = to_slots(factor * dx)
            sb2[pl.ds(2 + par, NT, stride=4), :] = to_slots(factor * dy)
            out_ref[0, :, lanes] = u
            out_ref[1, :, lanes] = v
        for chunk in range(4):
            send_chunk(sb, rb, sb_sem, rb_sem, chunk, 0)
        wait_bytes(ids.at[pl.ds(0, NT - 1)], id_send)
        for group, bufs in enumerate((ice_bufs, cur_bufs, push_bufs)):
            halo_sent(group, bufs)
        wait_bytes(sa.at[pl.ds(0, 448)], sa_sem)
        wait_bytes(sb, sb_sem)


def halo_scratch(count):
    size = 16 * count // 2
    return [
        *[pltpu.VMEM((count, 2, 256), F32)] * 4,
        *[pltpu.VMEM((size, 128), F32)] * 2,
        *[pltpu.VMEM((size + 16, 128), F32)] * 2,
    ]


def per_device(fields, block_owner, ice_covered, land_mask):
    out = pl.pallas_call(
        kernel,
        out_shape=jax.ShapeDtypeStruct((2, NT, 256), F32),
        in_specs=[pl.BlockSpec(memory_space=pltpu.HBM)] * 4,
        out_specs=pl.BlockSpec(memory_space=pltpu.VMEM),
        scratch_shapes=[
            pltpu.VMEM((7, NT, 256), F32),
            pltpu.VMEM((1, NT), jnp.int32),
            pltpu.VMEM((1, NT), jnp.int32),
            pltpu.VMEM((NT, 256), jnp.int32),
            pltpu.SemaphoreType.DMA((4,)),
            pltpu.VMEM((NT, 1, NT), jnp.int32),
            *[pltpu.VMEM((4 * NT, 1, 128), F32)] * 4,
            *[pltpu.VMEM((8 * NT, 1, 128), F32)] * 2,
            pltpu.VMEM((28, ROWS, 256), F32),
            pltpu.VMEM((NT, 256), F32),
            pltpu.VMEM((4, NT, 256), F32),
            pltpu.VMEM((2, NT, 256), F32),
            pltpu.VMEM((2, NT, 256), F32),
            pltpu.VMEM((2, NT, NT), F32),
            *halo_scratch(8),
            *halo_scratch(2),
            *halo_scratch(2),
            pltpu.SemaphoreType.DMA,
            pltpu.SemaphoreType.DMA,
            pltpu.SemaphoreType.DMA,
            pltpu.SemaphoreType.DMA((4,)),
            pltpu.SemaphoreType.DMA,
            pltpu.SemaphoreType.DMA((4,)),
            pltpu.SemaphoreType.DMA,
            pltpu.SemaphoreType.DMA((4,)),
            pltpu.SemaphoreType.DMA((24,)),
            pltpu.SemaphoreType.DMA((24,)),
        ],
        compiler_params=pltpu.CompilerParams(
            collective_id=0, has_side_effects=True, vmem_limit_bytes=60 * 1024 * 1024
        ),
    )(fields[0], block_owner.reshape(1, NT), ice_covered.reshape(1, NT), land_mask)
    return out[None]


def solution(mesh):
    placed = (
        P("comp", None, ("lat", "lon"), None),
        P(("lat", "lon")),
        P(("lat", "lon")),
        P(("lat", "lon"), None),
    )
    return jax.shard_map(
        per_device,
        mesh=mesh,
        in_specs=placed,
        out_specs=P("comp", None, ("lat", "lon"), None),
        check_vma=False,
    )
```

```python
import functools

import jax
import jax.numpy as jnp
from jax import lax
from jax.experimental import pallas as pl
from jax.experimental.pallas import tpu as pltpu
from jax.sharding import PartitionSpec as P


NSUB = 4
NLAT = 8
NLON = 16
NT = NLAT * NLON
TOP = 16
ROWS = 160
MESH = pl.DeviceIdType.MESH
HIGHEST = lax.Precision.HIGHEST
F32 = jnp.float32

U, V, S1, S2, S12, STR, MASS, DRAG, ACT, CX, CY, PX, PY, DEN, TURN = range(15)
DIRECT = 2
GROUP_ICE = (U, V, MASS, DRAG, S1, S2, S12, ACT)
GROUP_SEA = (CX, CY, PX, PY)


def lanes_of(shape):
    return lax.broadcasted_iota(jnp.int32, shape, len(shape) - 1)


def root(x):
    return x * lax.rsqrt(x)


def kernel(
    f_hbm, own_hbm, cov_hbm, land_hbm, out_ref,
    f_ref, own_ref, cov_ref, land_ref, in_sem,
    ids, sa, ra, sb, rb, sd, rd, x, act, gat, opn, outb, qmat,
    ss1, sn1, hs1, hn1, se1, sw1, pw1, pe1,
    ss2, sn2, hs2, hn2, se2, sw2, pw2, pe2,
    id_send, id_recv, sa_sem, ra_sem, sb_sem, rb_sem, sd_sem, rd_sem, h_send, h_recv,
):
    comp = lax.axis_index("comp")
    la = lax.axis_index("lat")
    lo = lax.axis_index("lon")
    me = la * NLON + lo
    barrier = pltpu.get_barrier_semaphore()
    sa2, ra2, sb2, rb2 = (r.reshape(4 * NT, 128) for r in (sa, ra, sb, rb))
    sd2, rd2 = (r.reshape(8 * NT, 128) for r in (sd, rd))

    loads = [
        pltpu.make_async_copy(src, dst, in_sem.at[n])
        for n, (src, dst) in enumerate(
            ((f_hbm, f_ref), (own_hbm, own_ref), (cov_hbm, cov_ref), (land_hbm, land_ref))
        )
    ]

    def greet(other):
        for tla in range(NLAT):
            for tlo in range(NLON):
                pl.semaphore_signal(barrier, inc=1, device_id=(other, tla, tlo), device_id_type=MESH)

    others = [lax.rem(lo + j, NLON) for j in range(NLON)]

    def target_lat(chunk, other):
        return lax.rem(la + (NLAT - chunk if other == 1 else chunk), NLAT)

    def send_chunk(src, dst, send_sem, recv_sem, chunk, other, stride=4, rows=4):
        tla = target_lat(chunk, other)
        for tlo in others:
            pltpu.make_async_remote_copy(
                src_ref=src.at[pl.ds(stride * (tla * NLON + tlo), rows)],
                dst_ref=dst.at[pl.ds(stride * me, rows)],
                send_sem=send_sem,
                recv_sem=recv_sem.at[chunk],
                device_id=(other, tla, tlo),
                device_id_type=MESH,
            ).start()

    def wait_bytes(ref, sem):
        pltpu.make_async_copy(ref, ref, sem).wait()

    def wait_chunk(dst, recv_sem, chunk, rows=4):
        wait_bytes(dst.at[pl.ds(0, NLON * rows)], recv_sem.at[chunk])

    def rows_of(chunk, half):
        return pl.multiple_of(target_lat(chunk, 1) * NLON + 8 * half, 8)

    @pl.when(comp == 0)
    def _():
        loads[0].start()
        greet(1)
        loads[0].wait()
        for ch in range(2):
            for par in range(2):
                sa2[pl.ds(2 * ch + par, NT, stride=4), :] = f_ref[2 + ch, :, pl.ds(128 * par, 128)]
        def air(k, carry):
            rows = pl.ds(pl.multiple_of(8 * k, 8), 8)
            wx, wy, cx, cy, rho = (f_ref[i, rows, :] for i in (0, 1, 2, 3, 6))
            scale = rho * 0.1 * root(wx * wx + wy * wy + 1.0)
            outb[0, rows, :] = scale * wx
            outb[1, rows, :] = scale * wy
            rx = wx - cx
            ry = wy - cy
            speed = root(rx * rx + ry * ry + 1.0)
            scale = rho * (0.1 + 0.05 * speed) * speed
            opn[0, rows, :] = scale * rx
            opn[1, rows, :] = scale * ry
            return carry

        lax.fori_loop(0, 16, air, 0)


        for chunk in range(DIRECT):
            for half in range(2):
                base = rows_of(chunk, half)
                for par in range(2):
                    lanes = pl.ds(128 * par, 128)
                    for ch in range(2):
                        sd2[pl.ds(8 * base + 2 * ch + par, 8, stride=8), :] = outb[ch, pl.ds(base, 8), lanes]
                        sd2[pl.ds(8 * base + 4 + 2 * ch + par, 8, stride=8), :] = f_ref[4 + ch, pl.ds(base, 8), lanes]

        pl.semaphore_wait(barrier, NT)
        for chunk in range(NLAT):
            send_chunk(sa, ra, sa_sem, ra_sem, chunk, 1)
        for chunk in range(DIRECT):
            send_chunk(sd, rd, sd_sem, rd_sem, chunk, 1, 8, 8)

        for chunk in range(DIRECT, NLAT):
            wait_chunk(ra, ra_sem, chunk)

            for half in range(2):
                base = rows_of(chunk, half)
                rows = pl.ds(base, 8)
                for par in range(2):
                    lanes = pl.ds(128 * par, 128)
                    conc = ra2[pl.ds(4 * base + par, 8, stride=4), :]
                    mass = ra2[pl.ds(4 * base + 2 + par, 8, stride=4), :]
                    for ch in range(2):
                        sb2[pl.ds(4 * base + 2 * ch + par, 8, stride=4), :] = (
                            conc * outb[ch, rows, lanes] - mass * f_ref[4 + ch, rows, lanes]
                        )
            send_chunk(sb, rb, sb_sem, rb_sem, chunk, 1)

        for chunk in range(NLAT):
            wait_chunk(rb, rb_sem, chunk)
        for chunk in range(DIRECT):
            wait_chunk(ra, ra_sem, chunk, 2)
        for ch in range(2):
            for par in range(2):
                lanes = pl.ds(128 * par, 128)
                conc = ra2[pl.ds(par, NT, stride=4), :]
                out_ref[ch, :, lanes] = rb2[pl.ds(2 * ch + par, NT, stride=4), :] + (1.0 - conc) * opn[ch, :, lanes]
        wait_bytes(sa, sa_sem)
        wait_bytes(sb.at[pl.ds(0, 4 * NLON * (NLAT - DIRECT))], sb_sem)
        wait_bytes(sd.at[pl.ds(0, 8 * NLON * DIRECT)], sd_sem)

    east = lax.rem(lo + 1, NLON)
    west = lax.rem(lo + NLON - 1, NLON)
    has_south = la > 0
    has_north = la < NLAT - 1

    def halo_copies(group, bufs):
        ss, sn, hs, hn, se, sw, pw, pe = bufs
        size = se.shape[0]
        south, north = la - 1, la + 1
        first, last = pl.ds(0, 8), pl.ds(size - 8, 8)
        below, middle, above = pl.ds(0, 8), pl.ds(8, size), pl.ds(8 + size, 8)
        plan = (
            (None, se, pw.at[middle], la, east),
            (None, sw, pe.at[middle], la, west),
            (has_north, sn, hs, north, lo),
            (has_north, se.at[last], pw.at[below], north, east),
            (has_north, sw.at[last], pe.at[below], north, west),
            (has_south, ss, hn, south, lo),
            (has_south, se.at[first], pw.at[above], south, east),
            (has_south, sw.at[first], pe.at[above], south, west),
        )
        return [
            (
                cond,
                pltpu.make_async_remote_copy(
                    src_ref=src, dst_ref=dst, send_sem=h_send.at[8 * group + n], recv_sem=h_recv.at[8 * group + n],
                    device_id=(1, tla, tlo), device_id_type=MESH,
                ),
            )
            for n, (cond, src, dst, tla, tlo) in enumerate(plan)
        ]

    def under(cond, action):
        if cond is None:
            action()
        else:
            pl.when(cond)(action)

    def halo_start(group, bufs, source):
        ss, sn, hs, hn, se, sw, pw, pe = bufs
        count, size = ss.shape[0], se.shape[0]
        for n in range(count):
            ss[n] = source(n)[pl.ds(0, 2), :]
            sn[n] = source(n)[pl.ds(126, 2), :]
        lane = lanes_of((size, 128))
        to_east = jnp.zeros((size, 128), F32)
        to_west = to_east
        for g in range(NT // size):
            for n in range(count):
                for par in range(2):
                    at = 8 * count * g + 8 * n + 4 * par
                    value = source(n)[pl.ds(size * g, size), pl.ds(128 * par, 128)]
                    here = (lane >= at) & (lane < at + 4)
                    to_west = jnp.where(here, pltpu.roll(value, at, 1) if at else value, to_west)
                    to_east = jnp.where(here, pltpu.roll(value, (at - 124) % 128, 1) if at != 124 else value, to_east)
        se[...] = to_east
        sw[...] = to_west
        for cond, copy in halo_copies(group, bufs):
            under(cond, copy.start)

    def halo_walls(bufs):
        ss, sn, hs, hn, se, sw, pw, pe = bufs
        size = se.shape[0]
        zero = jnp.zeros((8, 128), F32)

        @pl.when(la == 0)
        def _():
            hs[...] = jnp.zeros(hs.shape, F32)
            pw[pl.ds(0, 8), :] = zero
            pe[pl.ds(0, 8), :] = zero

        @pl.when(la == NLAT - 1)
        def _():
            hn[...] = jnp.zeros(hn.shape, F32)
            pw[pl.ds(8 + size, 8), :] = zero
            pe[pl.ds(8 + size, 8), :] = zero

    def halo_main(channels, source):
        for n, channel in enumerate(channels):
            for par in range(2):
                x[2 * channel + par, pl.ds(TOP, NT), pl.ds(0, 128)] = source(n)[:, pl.ds(128 * par, 128)]

    def halo_finish(group, bufs, channels):
        ss, sn, hs, hn, se, sw, pw, pe = bufs
        count, size = ss.shape[0], se.shape[0]
        copies = halo_copies(group, bufs)
        received = {2: has_south, 3: has_south, 4: has_south, 5: has_north, 6: has_north, 7: has_north}
        for n, (cond, copy) in enumerate(copies):
            under(received.get(n), copy.wait_recv)
        groups = NT // size
        parts = [(TOP + size * g, size, 8, g) for g in range(groups)]
        parts += [(8, 8, 0, groups - 1), (TOP + NT, 8, 8 + size, 0)]
        for start, rows, at, g in parts:
            from_west = pw[pl.ds(at, rows), :]
            from_east = pe[pl.ds(at, rows), :]
            lane = lanes_of((rows, 128))
            for n, channel in enumerate(channels):
                for par in range(2):
                    j = 8 * count * g + 8 * n + 4 * par
                    right = pltpu.roll(from_east, 128 - j, 1) if j else from_east
                    left = pltpu.roll(from_west, 124 - j, 1) if j != 124 else from_west
                    x[2 * channel + par, pl.ds(start, rows), pl.ds(128, 128)] = jnp.where(lane < 64, right, left)
        for n, channel in enumerate(channels):
            for par in range(2):
                lanes = pl.ds(128 * par, 128)
                x[2 * channel + par, pl.ds(TOP - 2, 2), pl.ds(0, 128)] = hs[n, :, lanes]
                x[2 * channel + par, pl.ds(TOP + NT, 2), pl.ds(0, 128)] = hn[n, :, lanes]

    def halo_sent(group, bufs):
        for cond, copy in halo_copies(group, bufs):
            under(cond, copy.wait_send)

    ice_bufs = (ss1, sn1, hs1, hn1, se1, sw1, pw1, pe1)
    sea_bufs = (ss2, sn2, hs2, hn2, se2, sw2, pw2, pe2)

    @pl.when(comp == 1)
    def _():
        for load in loads:
            load.start()
        rb[...] = jnp.zeros(rb.shape, F32)
        rd[...] = jnp.zeros(rd.shape, F32)
        greet(0)
        greet(1)
        for load in loads:
            load.wait()
        square = (NT, NT)
        diagonal = lax.broadcasted_iota(jnp.int32, square, 0) == lanes_of(square)
        covered = jnp.sum(jnp.where(diagonal, cov_ref[...].astype(F32), 0.0), axis=1, keepdims=True)
        act[...] = covered * (1 - land_ref[...]).astype(F32)
        halo_walls(ice_bufs)
        halo_walls(sea_bufs)

        pl.semaphore_wait(barrier, 2 * NT)

        def tell_one(tla, tlo):
            pltpu.make_async_remote_copy(
                src_ref=own_ref, dst_ref=ids.at[me], send_sem=id_send, recv_sem=id_recv,
                device_id=(1, tla, tlo), device_id_type=MESH,
            ).start()

        for tlo in others[1:]:
            tell_one(la, tlo)

        def tell(k, carry):
            tla = lax.rem(la + k, NLAT)
            for tlo in others:
                tell_one(tla, tlo)
            return carry

        lax.fori_loop(1, NLAT, tell, 0)
        ids[me] = own_ref[...]

        def ice_source(n):
            return f_ref.at[n] if n < 7 else act

        halo_start(0, ice_bufs, ice_source)

        wait_bytes(ids.at[pl.ds(0, NT - 1)], id_recv)
        every = ids.reshape(NT, NT)[...]
        local = jnp.where(lanes_of(square) == me, (every - NT * me).astype(F32), 0.0)
        local = jnp.sum(local, axis=1, keepdims=True)
        q = (local == lanes_of(square).astype(F32)).astype(F32)
        qmat[0] = q
        qmat[1] = q.T

        def to_slots(values):
            return jnp.dot(qmat[0], values, precision=HIGHEST, preferred_element_type=F32)

        def to_blocks(values):
            return jnp.dot(qmat[1], values, precision=HIGHEST, preferred_element_type=F32)

        a = act[...]
        for ch, value in enumerate((f_ref[3] * a, f_ref[2] * a)):
            moved = to_slots(value)
            for par in range(2):
                sa2[pl.ds(2 * ch + par, NT, stride=4), :] = moved[:, 128 * par : 128 * par + 128]
        for chunk in range(DIRECT, NLAT):
            send_chunk(sa, ra, sa_sem, ra_sem, chunk, 0)
        for chunk in range(DIRECT):
            send_chunk(sa, ra, sa_sem, ra_sem, chunk, 0, 4, 2)
        halo_main(GROUP_ICE, ice_source)
        halo_finish(0, ice_bufs, GROUP_ICE)

        def prepare(k, carry):
            rows = pl.ds(pl.multiple_of(48 * k + 8, 8), 48)
            for par in range(2):
                conc = x[2 * DRAG + par, rows, :]
                active = x[2 * ACT + par, rows, :]
                mass = x[2 * MASS + par, rows, :]
                x[2 * STR + par, rows, :] = mass * jnp.exp(2.0 * (conc - 1.0)) * (active * (1.0 / 6.0))
                x[2 * DRAG + par, rows, :] = 1.5 * conc * active
                x[2 * DEN + par, rows, :] = 2.0 * jnp.maximum(mass, 0.5)
                x[2 * TURN + par, rows, :] = 0.3 * mass
                x[2 * MASS + par, rows, :] = 2.0 * mass
                one = 0.5 * x[2 * S1 + par, rows, :]
                two = 0.5 * x[2 * S2 + par, rows, :]
                x[2 * S1 + par, rows, :] = one + two
                x[2 * S2 + par, rows, :] = one - two
            return carry

        lax.fori_loop(0, 3, prepare, 0)

        third = 1.0 / 1.5
        both = pl.ds(0, 256)

        def stress():
            for r in (8, 80):
                for par in range(2):
                    def get(channel, p=par, row=r):
                        return x[2 * channel + p, pl.ds(row, 72), :]

                    u, v = get(U), get(V)
                    un, vn = (get(c, 1) if par == 0 else get(c, 0, r + 1) for c in (U, V))
                    sxx = pltpu.roll(u, 255, 1) - u
                    syy = vn - v
                    shear = (un - u) + (pltpu.roll(v, 255, 1) - v)
                    div = sxx + syy
                    ten = sxx - syy
                    strength = get(STR)
                    visc = strength * lax.rsqrt(div * div + (ten * ten + shear * shear + 1.0) * 0.25)
                    quarter = 0.25 * visc
                    total = visc * div - strength
                    differ = quarter * ten
                    rows = pl.ds(r, 72)
                    x[2 * S1 + par, rows, :] = get(S1) * third + (total + differ)
                    x[2 * S2 + par, rows, :] = get(S2) * third + (total - differ)
                    x[2 * S12 + par, rows, :] = get(S12) * third + quarter * shear

        def momentum(r, n, half, final=False):
            lanes = both if half is None else pl.ds(128 * half, 128)
            for par in range(2):
                def get(channel, p=par, row=r, where=lanes):
                    return x[2 * channel + p, pl.ds(row, n), where]

                def west_of(channel):
                    rolled = pltpu.roll(get(channel), 1, 1)
                    if half is None:
                        return rolled
                    beyond = pltpu.roll(get(channel, where=pl.ds(128 - 128 * half, 128)), 1, 1)
                    return jnp.where(lanes_of((n, 128)) == 0, beyond, rolled)

                s12 = get(S12)
                south = (1, r - 1) if par == 0 else (0, r)
                force_x = get(S1) - west_of(S1) + (s12 - get(S12, *south))
                force_y = s12 - west_of(S12) + (get(S2) - get(S2, *south))
                u, v, cx, cy, mass2, turn = (get(c) for c in (U, V, CX, CY, MASS, TURN))
                dx = cx - u
                dy = cy - v
                base = get(DRAG)
                drag = base * root(dx * dx + dy * dy + 0.1)
                scale = get(ACT) / (get(DEN) + drag)
                unew = scale * (mass2 * u + force_x + get(PX) + drag * cx + turn * v)
                vnew = scale * (mass2 * v + force_y + get(PY) + drag * cy - turn * u)
                if final:
                    rows, place = pl.ds(r - TOP, n), pl.ds(128 * par, 128)
                    out_ref[0, rows, place] = unew
                    out_ref[1, rows, place] = vnew
                    dx = unew - cx
                    dy = vnew - cy
                    factor = base * root(dx * dx + dy * dy + 0.1)
                    gat[0, rows, place] = factor * dx
                    gat[1, rows, place] = factor * dy
                else:
                    x[2 * U + par, pl.ds(r, n), lanes] = unew
                    x[2 * V + par, pl.ds(r, n), lanes] = vnew

        stress()

        for chunk in range(NLAT):
            wait_chunk(ra, ra_sem, chunk)
        for ch in range(2):
            for par in range(2):
                gat[ch, :, pl.ds(128 * par, 128)] = to_blocks(ra2[pl.ds(2 * ch + par, NT, stride=4), :])
        for chunk in range(DIRECT):
            wait_chunk(rd, rd_sem, chunk, 8)
        for par in range(2):
            lanes = pl.ds(128 * par, 128)
            for ch in range(2):
                stress_of_air = to_blocks(rd2[pl.ds(2 * ch + par, NT, stride=8), :])
                tilt = to_blocks(rd2[pl.ds(4 + 2 * ch + par, NT, stride=8), :])
                gat[2 + ch, :, lanes] = act[:, lanes] * (f_ref[3, :, lanes] * stress_of_air - f_ref[2, :, lanes] * tilt)
        for chunk in range(DIRECT, NLAT):
            wait_chunk(rb, rb_sem, chunk)
        for ch in range(2):
            for par in range(2):
                gat[2 + ch, :, pl.ds(128 * par, 128)] += to_blocks(rb2[pl.ds(2 * ch + par, NT, stride=4), :])
        halo_start(1, sea_bufs, lambda n: gat.at[n])
        halo_main(GROUP_SEA, lambda n: gat.at[n])
        momentum(TOP, 64, 0)
        momentum(TOP + 64, 64, 0)
        halo_finish(1, sea_bufs, GROUP_SEA)
        momentum(8, 8, 0)
        momentum(TOP + NT, 8, 0)
        momentum(8, 144, 1)
        for repeat in range(NSUB - 2):
            stress()
            momentum(8, 72, None)
            momentum(80, 72, None)
        stress()
        momentum(TOP, 64, 0, True)
        momentum(TOP + 64, 64, 0, True)
        for ch in range(2):
            for par in range(2):
                sb2[pl.ds(2 * ch + par, NT, stride=4), :] = to_slots(gat[ch, :, pl.ds(128 * par, 128)])
        for chunk in range(NLAT):
            send_chunk(sb, rb, sb_sem, rb_sem, chunk, 0)
        wait_bytes(ids.at[pl.ds(0, NT - 1)], id_send)
        for group, bufs in enumerate((ice_bufs, sea_bufs)):
            halo_sent(group, bufs)
        wait_bytes(sa.at[pl.ds(0, 4 * NT - 2 * NLON * DIRECT)], sa_sem)
        wait_bytes(sb, sb_sem)


def halo_scratch(count):
    size = 16 * count // 2
    return [
        *[pltpu.VMEM((count, 2, 256), F32)] * 4,
        *[pltpu.VMEM((size, 128), F32)] * 2,
        *[pltpu.VMEM((size + 16, 128), F32)] * 2,
    ]


def per_device(fields, block_owner, ice_covered, land_mask):
    out = pl.pallas_call(
        kernel,
        out_shape=jax.ShapeDtypeStruct((2, NT, 256), F32),
        in_specs=[pl.BlockSpec(memory_space=pltpu.HBM)] * 4,
        out_specs=pl.BlockSpec(memory_space=pltpu.VMEM),
        scratch_shapes=[
            pltpu.VMEM((7, NT, 256), F32),
            pltpu.VMEM((1, NT), jnp.int32),
            pltpu.VMEM((1, NT), jnp.int32),
            pltpu.VMEM((NT, 256), jnp.int32),
            pltpu.SemaphoreType.DMA((4,)),
            pltpu.VMEM((NT, 1, NT), jnp.int32),
            *[pltpu.VMEM((4 * NT, 1, 128), F32)] * 4,
            *[pltpu.VMEM((8 * NT, 1, 128), F32)] * 2,
            pltpu.VMEM((30, ROWS, 256), F32),
            pltpu.VMEM((NT, 256), F32),
            pltpu.VMEM((4, NT, 256), F32),
            pltpu.VMEM((2, NT, 256), F32),
            pltpu.VMEM((2, NT, 256), F32),
            pltpu.VMEM((2, NT, NT), F32),
            *halo_scratch(8),
            *halo_scratch(4),
            pltpu.SemaphoreType.DMA,
            pltpu.SemaphoreType.DMA,
            pltpu.SemaphoreType.DMA,
            pltpu.SemaphoreType.DMA((NLAT,)),
            pltpu.SemaphoreType.DMA,
            pltpu.SemaphoreType.DMA((NLAT,)),
            pltpu.SemaphoreType.DMA,
            pltpu.SemaphoreType.DMA((NLAT,)),
            pltpu.SemaphoreType.DMA((16,)),
            pltpu.SemaphoreType.DMA((16,)),
        ],
        compiler_params=pltpu.CompilerParams(
            collective_id=0, has_side_effects=True, vmem_limit_bytes=40 * 1024 * 1024
        ),
    )(
        *(
            pltpu.with_memory_space_constraint(a, pltpu.HBM)
            for a in (fields[0], block_owner.reshape(1, NT), ice_covered.reshape(1, NT), land_mask)
        )
    )
    return out[None]


def solution(mesh):
    placed = (
        P("comp", None, ("lat", "lon"), None),
        P(("lat", "lon")),
        P(("lat", "lon")),
        P(("lat", "lon"), None),
    )
    return jax.shard_map(
        per_device,
        mesh=mesh,
        in_specs=placed,
        out_specs=P("comp", None, ("lat", "lon"), None),
        check_vma=False,
    )
```

```python
import functools

import jax
import jax.numpy as jnp
from jax import lax
from jax.experimental import pallas as pl
from jax.experimental.pallas import tpu as pltpu
from jax.sharding import PartitionSpec as P


NSUB = 4
NLAT = 8
NLON = 16
NT = NLAT * NLON
TOP = 16
ROWS = 160
MESH = pl.DeviceIdType.MESH
HIGHEST = lax.Precision.HIGHEST
F32 = jnp.float32

U, V, S1, S2, S12, STR, MASS, DRAG, ACT, CX, CY, PX, PY, DEN, TURN = range(15)
DIRECT = 2
GROUP_ICE = (U, V, MASS, DRAG, S1, S2, S12, ACT)
GROUP_SEA = (CX, CY, PX, PY)


def lanes_of(shape):
    return lax.broadcasted_iota(jnp.int32, shape, len(shape) - 1)


def root(x):
    return x * lax.rsqrt(x)


def kernel(
    f_hbm, own_hbm, cov_hbm, land_hbm, out_ref,
    f_ref, own_ref, cov_ref, land_ref, in_sem,
    ids, sa, ra, sb, rb, sd, rd, x, act, gat, opn, outb, qmat,
    ss1, sn1, hs1, hn1, se1, sw1, pw1, pe1,
    ss2, sn2, hs2, hn2, se2, sw2, pw2, pe2,
    id_send, id_recv, sa_sem, ra_sem, sb_sem, rb_sem, sd_sem, rd_sem, h_send, h_recv,
):
    comp = lax.axis_index("comp")
    la = lax.axis_index("lat")
    lo = lax.axis_index("lon")
    me = la * NLON + lo
    barrier = pltpu.get_barrier_semaphore()
    sa2, ra2, sb2, rb2 = (r.reshape(4 * NT, 128) for r in (sa, ra, sb, rb))
    sd2, rd2 = (r.reshape(8 * NT, 128) for r in (sd, rd))

    loads = [
        pltpu.make_async_copy(src, dst, in_sem.at[n])
        for n, (src, dst) in enumerate(
            ((f_hbm, f_ref), (own_hbm, own_ref), (cov_hbm, cov_ref), (land_hbm, land_ref))
        )
    ]

    def greet(other):
        for tla in range(NLAT):
            for tlo in range(NLON):
                pl.semaphore_signal(barrier, inc=1, device_id=(other, tla, tlo), device_id_type=MESH)

    others = [lax.rem(lo + j, NLON) for j in range(NLON)]

    def target_lat(chunk, other):
        return lax.rem(la + (NLAT - chunk if other == 1 else chunk), NLAT)

    def send_chunk(src, dst, send_sem, recv_sem, chunk, other, stride=4, rows=4):
        tla = target_lat(chunk, other)
        for tlo in others:
            pltpu.make_async_remote_copy(
                src_ref=src.at[pl.ds(stride * (tla * NLON + tlo), rows)],
                dst_ref=dst.at[pl.ds(stride * me, rows)],
                send_sem=send_sem,
                recv_sem=recv_sem.at[chunk],
                device_id=(other, tla, tlo),
                device_id_type=MESH,
            ).start()

    def wait_bytes(ref, sem):
        pltpu.make_async_copy(ref, ref, sem).wait()

    def wait_chunk(dst, recv_sem, chunk, rows=4):
        wait_bytes(dst.at[pl.ds(0, NLON * rows)], recv_sem.at[chunk])

    def rows_of(chunk, half):
        return pl.multiple_of(target_lat(chunk, 1) * NLON + 8 * half, 8)

    @pl.when(comp == 0)
    def _():
        loads[0].start()
        greet(1)
        loads[0].wait()
        for ch in range(2):
            for par in range(2):
                sa2[pl.ds(2 * ch + par, NT, stride=4), :] = f_ref[2 + ch, :, pl.ds(128 * par, 128)]
        def air(k, carry):
            rows = pl.ds(pl.multiple_of(8 * k, 8), 8)
            wx, wy, cx, cy, rho = (f_ref[i, rows, :] for i in (0, 1, 2, 3, 6))
            scale = rho * 0.1 * root(wx * wx + wy * wy + 1.0)
            outb[0, rows, :] = scale * wx
            outb[1, rows, :] = scale * wy
            rx = wx - cx
            ry = wy - cy
            speed = root(rx * rx + ry * ry + 1.0)
            scale = rho * (0.1 + 0.05 * speed) * speed
            opn[0, rows, :] = scale * rx
            opn[1, rows, :] = scale * ry
            return carry

        lax.fori_loop(0, 16, air, 0)


        for chunk in range(DIRECT):
            for half in range(2):
                base = rows_of(chunk, half)
                for par in range(2):
                    lanes = pl.ds(128 * par, 128)
                    for ch in range(2):
                        sd2[pl.ds(8 * base + 2 * ch + par, 8, stride=8), :] = outb[ch, pl.ds(base, 8), lanes]
                        sd2[pl.ds(8 * base + 4 + 2 * ch + par, 8, stride=8), :] = f_ref[4 + ch, pl.ds(base, 8), lanes]

        pl.semaphore_wait(barrier, NT)
        for chunk in range(NLAT):
            send_chunk(sa, ra, sa_sem, ra_sem, chunk, 1)
        for chunk in range(DIRECT):
            send_chunk(sd, rd, sd_sem, rd_sem, chunk, 1, 8, 8)

        for chunk in range(DIRECT, NLAT):
            wait_chunk(ra, ra_sem, chunk)

            for half in range(2):
                base = rows_of(chunk, half)
                rows = pl.ds(base, 8)
                for par in range(2):
                    lanes = pl.ds(128 * par, 128)
                    conc = ra2[pl.ds(4 * base + par, 8, stride=4), :]
                    mass = ra2[pl.ds(4 * base + 2 + par, 8, stride=4), :]
                    for ch in range(2):
                        sb2[pl.ds(4 * base + 2 * ch + par, 8, stride=4), :] = (
                            conc * outb[ch, rows, lanes] - mass * f_ref[4 + ch, rows, lanes]
                        )
            send_chunk(sb, rb, sb_sem, rb_sem, chunk, 1)

        for chunk in range(DIRECT):
            wait_chunk(ra, ra_sem, chunk, 2)
        for chunk in range(NLAT):
            wait_chunk(rb, rb_sem, chunk)
            base = rows_of(chunk, 0)
            rows = pl.ds(base, NLON)
            for par in range(2):
                lanes = pl.ds(128 * par, 128)
                rest = 1.0 - ra2[pl.ds(4 * base + par, NLON, stride=4), :]
                for ch in range(2):
                    out_ref[ch, rows, lanes] = (
                        rb2[pl.ds(4 * base + 2 * ch + par, NLON, stride=4), :] + rest * opn[ch, rows, lanes]
                    )
        wait_bytes(sa, sa_sem)
        wait_bytes(sb.at[pl.ds(0, 4 * NLON * (NLAT - DIRECT))], sb_sem)
        wait_bytes(sd.at[pl.ds(0, 8 * NLON * DIRECT)], sd_sem)

    east = lax.rem(lo + 1, NLON)
    west = lax.rem(lo + NLON - 1, NLON)
    has_south = la > 0
    has_north = la < NLAT - 1

    def halo_copies(group, bufs):
        ss, sn, hs, hn, se, sw, pw, pe = bufs
        size = se.shape[0]
        south, north = la - 1, la + 1
        first, last = pl.ds(0, 8), pl.ds(size - 8, 8)
        below, middle, above = pl.ds(0, 8), pl.ds(8, size), pl.ds(8 + size, 8)
        plan = (
            (None, se, pw.at[middle], la, east),
            (None, sw, pe.at[middle], la, west),
            (has_north, sn, hs, north, lo),
            (has_north, se.at[last], pw.at[below], north, east),
            (has_north, sw.at[last], pe.at[below], north, west),
            (has_south, ss, hn, south, lo),
            (has_south, se.at[first], pw.at[above], south, east),
            (has_south, sw.at[first], pe.at[above], south, west),
        )
        return [
            (
                cond,
                pltpu.make_async_remote_copy(
                    src_ref=src, dst_ref=dst, send_sem=h_send.at[8 * group + n], recv_sem=h_recv.at[8 * group + n],
                    device_id=(1, tla, tlo), device_id_type=MESH,
                ),
            )
            for n, (cond, src, dst, tla, tlo) in enumerate(plan)
        ]

    def under(cond, action):
        if cond is None:
            action()
        else:
            pl.when(cond)(action)

    def halo_start(group, bufs, source):
        ss, sn, hs, hn, se, sw, pw, pe = bufs
        count, size = ss.shape[0], se.shape[0]
        for n in range(count):
            ss[n] = source(n)[pl.ds(0, 2), :]
            sn[n] = source(n)[pl.ds(126, 2), :]
        lane = lanes_of((size, 128))
        to_east = jnp.zeros((size, 128), F32)
        to_west = to_east
        for g in range(NT // size):
            for n in range(count):
                for par in range(2):
                    at = 8 * count * g + 8 * n + 4 * par
                    value = source(n)[pl.ds(size * g, size), pl.ds(128 * par, 128)]
                    here = (lane >= at) & (lane < at + 4)
                    to_west = jnp.where(here, pltpu.roll(value, at, 1) if at else value, to_west)
                    to_east = jnp.where(here, pltpu.roll(value, (at - 124) % 128, 1) if at != 124 else value, to_east)
        se[...] = to_east
        sw[...] = to_west
        for cond, copy in halo_copies(group, bufs):
            under(cond, copy.start)

    def halo_walls(bufs):
        ss, sn, hs, hn, se, sw, pw, pe = bufs
        size = se.shape[0]
        zero = jnp.zeros((8, 128), F32)

        @pl.when(la == 0)
        def _():
            hs[...] = jnp.zeros(hs.shape, F32)
            pw[pl.ds(0, 8), :] = zero
            pe[pl.ds(0, 8), :] = zero

        @pl.when(la == NLAT - 1)
        def _():
            hn[...] = jnp.zeros(hn.shape, F32)
            pw[pl.ds(8 + size, 8), :] = zero
            pe[pl.ds(8 + size, 8), :] = zero

    def halo_main(channels, source):
        for n, channel in enumerate(channels):
            for par in range(2):
                x[2 * channel + par, pl.ds(TOP, NT), pl.ds(0, 128)] = source(n)[:, pl.ds(128 * par, 128)]

    def halo_finish(group, bufs, channels):
        ss, sn, hs, hn, se, sw, pw, pe = bufs
        count, size = ss.shape[0], se.shape[0]
        copies = halo_copies(group, bufs)
        received = {2: has_south, 3: has_south, 4: has_south, 5: has_north, 6: has_north, 7: has_north}
        for n, (cond, copy) in enumerate(copies):
            under(received.get(n), copy.wait_recv)
        groups = NT // size
        parts = [(TOP + size * g, size, 8, g) for g in range(groups)]
        parts += [(8, 8, 0, groups - 1), (TOP + NT, 8, 8 + size, 0)]
        for start, rows, at, g in parts:
            from_west = pw[pl.ds(at, rows), :]
            from_east = pe[pl.ds(at, rows), :]
            lane = lanes_of((rows, 128))
            for n, channel in enumerate(channels):
                for par in range(2):
                    j = 8 * count * g + 8 * n + 4 * par
                    right = pltpu.roll(from_east, 128 - j, 1) if j else from_east
                    left = pltpu.roll(from_west, 124 - j, 1) if j != 124 else from_west
                    x[2 * channel + par, pl.ds(start, rows), pl.ds(128, 128)] = jnp.where(lane < 64, right, left)
        for n, channel in enumerate(channels):
            for par in range(2):
                lanes = pl.ds(128 * par, 128)
                x[2 * channel + par, pl.ds(TOP - 2, 2), pl.ds(0, 128)] = hs[n, :, lanes]
                x[2 * channel + par, pl.ds(TOP + NT, 2), pl.ds(0, 128)] = hn[n, :, lanes]

    def halo_sent(group, bufs):
        for cond, copy in halo_copies(group, bufs):
            under(cond, copy.wait_send)

    ice_bufs = (ss1, sn1, hs1, hn1, se1, sw1, pw1, pe1)
    sea_bufs = (ss2, sn2, hs2, hn2, se2, sw2, pw2, pe2)

    @pl.when(comp == 1)
    def _():
        for load in loads:
            load.start()
        greet(0)
        greet(1)
        for chunk in range(NLAT):
            first = lax.rem(la + chunk, NLAT) * NLON
            if chunk < DIRECT:
                rb[pl.ds(4 * first, 4 * NLON)] = jnp.zeros((4 * NLON, 1, 128), F32)
            else:
                rd[pl.ds(8 * first, 8 * NLON)] = jnp.zeros((8 * NLON, 1, 128), F32)
        for load in loads:
            load.wait()
        square = (NT, NT)
        diagonal = lax.broadcasted_iota(jnp.int32, square, 0) == lanes_of(square)
        covered = jnp.sum(jnp.where(diagonal, cov_ref[...].astype(F32), 0.0), axis=1, keepdims=True)
        act[...] = covered * (1 - land_ref[...]).astype(F32)
        halo_walls(ice_bufs)
        halo_walls(sea_bufs)

        pl.semaphore_wait(barrier, 2 * NT)

        def tell_one(tla, tlo):
            pltpu.make_async_remote_copy(
                src_ref=own_ref, dst_ref=ids.at[me], send_sem=id_send, recv_sem=id_recv,
                device_id=(1, tla, tlo), device_id_type=MESH,
            ).start()

        for tlo in others[1:]:
            tell_one(la, tlo)

        def tell(k, carry):
            tla = lax.rem(la + k, NLAT)
            for tlo in others:
                tell_one(tla, tlo)
            return carry

        lax.fori_loop(1, NLAT, tell, 0)
        ids[me] = own_ref[...]

        def ice_source(n):
            return f_ref.at[n] if n < 7 else act

        halo_start(0, ice_bufs, ice_source)

        wait_bytes(ids.at[pl.ds(0, NT - 1)], id_recv)
        every = ids.reshape(NT, NT)[...]
        local = jnp.where(lanes_of(square) == me, (every - NT * me).astype(F32), 0.0)
        local = jnp.sum(local, axis=1, keepdims=True)
        q = (local == lanes_of(square).astype(F32)).astype(F32)
        qmat[0] = q
        qmat[1] = q.T

        def to_slots(values):
            return jnp.dot(qmat[0], values, precision=HIGHEST, preferred_element_type=F32)

        def to_blocks(values):
            return jnp.dot(qmat[1], values, precision=HIGHEST, preferred_element_type=F32)

        a = act[...]
        for ch, value in enumerate((f_ref[3] * a, f_ref[2] * a)):
            moved = to_slots(value)
            for par in range(2):
                sa2[pl.ds(2 * ch + par, NT, stride=4), :] = moved[:, 128 * par : 128 * par + 128]
        for chunk in range(DIRECT, NLAT):
            send_chunk(sa, ra, sa_sem, ra_sem, chunk, 0)
        for chunk in range(DIRECT):
            send_chunk(sa, ra, sa_sem, ra_sem, chunk, 0, 4, 2)
        halo_main(GROUP_ICE, ice_source)
        halo_finish(0, ice_bufs, GROUP_ICE)

        def prepare(k, carry):
            rows = pl.ds(pl.multiple_of(48 * k + 8, 8), 48)
            for par in range(2):
                conc = x[2 * DRAG + par, rows, :]
                active = x[2 * ACT + par, rows, :]
                mass = x[2 * MASS + par, rows, :]
                x[2 * STR + par, rows, :] = mass * jnp.exp(2.0 * (conc - 1.0)) * (active * (1.0 / 6.0))
                x[2 * DRAG + par, rows, :] = 1.5 * conc * active
                x[2 * DEN + par, rows, :] = 2.0 * jnp.maximum(mass, 0.5)
                x[2 * TURN + par, rows, :] = 0.3 * mass
                x[2 * MASS + par, rows, :] = 2.0 * mass
                one = 0.5 * x[2 * S1 + par, rows, :]
                two = 0.5 * x[2 * S2 + par, rows, :]
                x[2 * S1 + par, rows, :] = one + two
                x[2 * S2 + par, rows, :] = one - two
            return carry

        lax.fori_loop(0, 3, prepare, 0)

        third = 1.0 / 1.5
        both = pl.ds(0, 256)

        def stress():
            for r in (8, 80):
                for par in range(2):
                    def get(channel, p=par, row=r):
                        return x[2 * channel + p, pl.ds(row, 72), :]

                    u, v = get(U), get(V)
                    un, vn = (get(c, 1) if par == 0 else get(c, 0, r + 1) for c in (U, V))
                    sxx = pltpu.roll(u, 255, 1) - u
                    syy = vn - v
                    shear = (un - u) + (pltpu.roll(v, 255, 1) - v)
                    div = sxx + syy
                    ten = sxx - syy
                    strength = get(STR)
                    visc = strength * lax.rsqrt(div * div + (ten * ten + shear * shear + 1.0) * 0.25)
                    quarter = 0.25 * visc
                    total = visc * div - strength
                    differ = quarter * ten
                    rows = pl.ds(r, 72)
                    x[2 * S1 + par, rows, :] = get(S1) * third + (total + differ)
                    x[2 * S2 + par, rows, :] = get(S2) * third + (total - differ)
                    x[2 * S12 + par, rows, :] = get(S12) * third + quarter * shear

        def momentum(r, n, half, final=False):
            lanes = both if half is None else pl.ds(128 * half, 128)
            for par in range(2):
                def get(channel, p=par, row=r, where=lanes):
                    return x[2 * channel + p, pl.ds(row, n), where]

                def west_of(channel):
                    rolled = pltpu.roll(get(channel), 1, 1)
                    if half is None:
                        return rolled
                    beyond = pltpu.roll(get(channel, where=pl.ds(128 - 128 * half, 128)), 1, 1)
                    return jnp.where(lanes_of((n, 128)) == 0, beyond, rolled)

                s12 = get(S12)
                south = (1, r - 1) if par == 0 else (0, r)
                force_x = get(S1) - west_of(S1) + (s12 - get(S12, *south))
                force_y = s12 - west_of(S12) + (get(S2) - get(S2, *south))
                u, v, cx, cy, mass2, turn = (get(c) for c in (U, V, CX, CY, MASS, TURN))
                dx = cx - u
                dy = cy - v
                base = get(DRAG)
                drag = base * root(dx * dx + dy * dy + 0.1)
                scale = get(ACT) / (get(DEN) + drag)
                unew = scale * (mass2 * u + force_x + get(PX) + drag * cx + turn * v)
                vnew = scale * (mass2 * v + force_y + get(PY) + drag * cy - turn * u)
                if final:
                    rows, place = pl.ds(r - TOP, n), pl.ds(128 * par, 128)
                    out_ref[0, rows, place] = unew
                    out_ref[1, rows, place] = vnew
                    dx = unew - cx
                    dy = vnew - cy
                    factor = base * root(dx * dx + dy * dy + 0.1)
                    gat[0, rows, place] = factor * dx
                    gat[1, rows, place] = factor * dy
                else:
                    x[2 * U + par, pl.ds(r, n), lanes] = unew
                    x[2 * V + par, pl.ds(r, n), lanes] = vnew

        stress()

        for chunk in range(NLAT):
            wait_chunk(ra, ra_sem, chunk)
        for ch in range(2):
            for par in range(2):
                gat[ch, :, pl.ds(128 * par, 128)] = to_blocks(ra2[pl.ds(2 * ch + par, NT, stride=4), :])
        for chunk in range(DIRECT):
            wait_chunk(rd, rd_sem, chunk, 8)
        for par in range(2):
            lanes = pl.ds(128 * par, 128)
            for ch in range(2):
                stress_of_air = to_blocks(rd2[pl.ds(2 * ch + par, NT, stride=8), :])
                tilt = to_blocks(rd2[pl.ds(4 + 2 * ch + par, NT, stride=8), :])
                gat[2 + ch, :, lanes] = act[:, lanes] * (f_ref[3, :, lanes] * stress_of_air - f_ref[2, :, lanes] * tilt)
        for chunk in range(DIRECT, NLAT):
            wait_chunk(rb, rb_sem, chunk)
        for ch in range(2):
            for par in range(2):
                gat[2 + ch, :, pl.ds(128 * par, 128)] += to_blocks(rb2[pl.ds(2 * ch + par, NT, stride=4), :])
        halo_start(1, sea_bufs, lambda n: gat.at[n])
        halo_main(GROUP_SEA, lambda n: gat.at[n])
        momentum(TOP, 64, 0)
        momentum(TOP + 64, 64, 0)
        halo_finish(1, sea_bufs, GROUP_SEA)
        momentum(8, 8, 0)
        momentum(TOP + NT, 8, 0)
        momentum(8, 144, 1)
        for repeat in range(NSUB - 2):
            stress()
            momentum(8, 72, None)
            momentum(80, 72, None)
        stress()
        momentum(TOP, 64, 0, True)
        momentum(TOP + 64, 64, 0, True)
        for ch in range(2):
            for par in range(2):
                sb2[pl.ds(2 * ch + par, NT, stride=4), :] = to_slots(gat[ch, :, pl.ds(128 * par, 128)])
        for chunk in range(NLAT):
            send_chunk(sb, rb, sb_sem, rb_sem, chunk, 0)
        wait_bytes(ids.at[pl.ds(0, NT - 1)], id_send)
        for group, bufs in enumerate((ice_bufs, sea_bufs)):
            halo_sent(group, bufs)
        wait_bytes(sa.at[pl.ds(0, 4 * NT - 2 * NLON * DIRECT)], sa_sem)
        wait_bytes(sb, sb_sem)


def halo_scratch(count):
    size = 16 * count // 2
    return [
        *[pltpu.VMEM((count, 2, 256), F32)] * 4,
        *[pltpu.VMEM((size, 128), F32)] * 2,
        *[pltpu.VMEM((size + 16, 128), F32)] * 2,
    ]


def per_device(fields, block_owner, ice_covered, land_mask):
    out = pl.pallas_call(
        kernel,
        out_shape=jax.ShapeDtypeStruct((2, NT, 256), F32),
        in_specs=[pl.BlockSpec(memory_space=pltpu.HBM)] * 4,
        out_specs=pl.BlockSpec(memory_space=pltpu.VMEM),
        scratch_shapes=[
            pltpu.VMEM((7, NT, 256), F32),
            pltpu.VMEM((1, NT), jnp.int32),
            pltpu.VMEM((1, NT), jnp.int32),
            pltpu.VMEM((NT, 256), jnp.int32),
            pltpu.SemaphoreType.DMA((4,)),
            pltpu.VMEM((NT, 1, NT), jnp.int32),
            *[pltpu.VMEM((4 * NT, 1, 128), F32)] * 4,
            *[pltpu.VMEM((8 * NT, 1, 128), F32)] * 2,
            pltpu.VMEM((30, ROWS, 256), F32),
            pltpu.VMEM((NT, 256), F32),
            pltpu.VMEM((4, NT, 256), F32),
            pltpu.VMEM((2, NT, 256), F32),
            pltpu.VMEM((2, NT, 256), F32),
            pltpu.VMEM((2, NT, NT), F32),
            *halo_scratch(8),
            *halo_scratch(4),
            pltpu.SemaphoreType.DMA,
            pltpu.SemaphoreType.DMA,
            pltpu.SemaphoreType.DMA,
            pltpu.SemaphoreType.DMA((NLAT,)),
            pltpu.SemaphoreType.DMA,
            pltpu.SemaphoreType.DMA((NLAT,)),
            pltpu.SemaphoreType.DMA,
            pltpu.SemaphoreType.DMA((NLAT,)),
            pltpu.SemaphoreType.DMA((16,)),
            pltpu.SemaphoreType.DMA((16,)),
        ],
        compiler_params=pltpu.CompilerParams(
            collective_id=0, has_side_effects=True, vmem_limit_bytes=40 * 1024 * 1024
        ),
    )(
        *(
            pltpu.with_memory_space_constraint(a, pltpu.HBM)
            for a in (fields[0], block_owner.reshape(1, NT), ice_covered.reshape(1, NT), land_mask)
        )
    )
    return out[None]


def solution(mesh):
    placed = (
        P("comp", None, ("lat", "lon"), None),
        P(("lat", "lon")),
        P(("lat", "lon")),
        P(("lat", "lon"), None),
    )
    return jax.shard_map(
        per_device,
        mesh=mesh,
        in_specs=placed,
        out_specs=P("comp", None, ("lat", "lon"), None),
        check_vma=False,
    )
```

```python
import functools

import jax
import jax.numpy as jnp
from jax import lax
from jax.experimental import pallas as pl
from jax.experimental.pallas import tpu as pltpu
from jax.sharding import PartitionSpec as P


NSUB = 4
NLAT = 8
NLON = 16
NT = NLAT * NLON
TOP = 16
ROWS = 160
MESH = pl.DeviceIdType.MESH
HIGHEST = lax.Precision.HIGHEST
F32 = jnp.float32

U, V, S1, S2, S12, STR, MASS, DRAG, ACT, CX, CY, PX, PY, DEN, TURN = range(15)
DIRECT = 2
GROUP_ICE = (U, V, MASS, DRAG, S1, S2, S12, ACT)
GROUP_SEA = (CX, CY, PX, PY)


def lanes_of(shape):
    return lax.broadcasted_iota(jnp.int32, shape, len(shape) - 1)


def root(x):
    return x * lax.rsqrt(x)


def kernel(
    f_hbm, own_hbm, cov_hbm, land_hbm, out_ref,
    f_ref, own_ref, cov_ref, land_ref, in_sem,
    ids, sa, ra, sb, rb, sd, rd, x, act, gat, opn, outb, qmat,
    ss1, sn1, hs1, hn1, se1, sw1, pw1, pe1,
    ss2, sn2, hs2, hn2, se2, sw2, pw2, pe2,
    id_send, id_recv, sa_sem, ra_sem, sb_sem, rb_sem, sd_sem, rd_sem, h_send, h_recv,
):
    comp = lax.axis_index("comp")
    la = lax.axis_index("lat")
    lo = lax.axis_index("lon")
    me = la * NLON + lo
    barrier = pltpu.get_barrier_semaphore()
    sa2, ra2, sb2, rb2 = (r.reshape(4 * NT, 128) for r in (sa, ra, sb, rb))
    sd2, rd2 = (r.reshape(8 * NT, 128) for r in (sd, rd))

    loads = [
        pltpu.make_async_copy(src, dst, in_sem.at[n])
        for n, (src, dst) in enumerate(
            ((f_hbm, f_ref), (own_hbm, own_ref), (cov_hbm, cov_ref), (land_hbm, land_ref))
        )
    ]

    def greet(other):
        for tla in range(NLAT):
            for tlo in range(NLON):
                pl.semaphore_signal(barrier, inc=1, device_id=(other, tla, tlo), device_id_type=MESH)

    others = [lax.rem(lo + j, NLON) for j in range(NLON)]

    def target_lat(chunk, other):
        return lax.rem(la + (NLAT - chunk if other == 1 else chunk), NLAT)

    def send_chunk(src, dst, send_sem, recv_sem, chunk, other, stride=4, rows=4):
        tla = target_lat(chunk, other)
        for tlo in others:
            pltpu.make_async_remote_copy(
                src_ref=src.at[pl.ds(stride * (tla * NLON + tlo), rows)],
                dst_ref=dst.at[pl.ds(stride * me, rows)],
                send_sem=send_sem,
                recv_sem=recv_sem.at[chunk],
                device_id=(other, tla, tlo),
                device_id_type=MESH,
            ).start()

    def wait_bytes(ref, sem):
        pltpu.make_async_copy(ref, ref, sem).wait()

    def wait_chunk(dst, recv_sem, chunk, rows=4):
        wait_bytes(dst.at[pl.ds(0, NLON * rows)], recv_sem.at[chunk])

    def rows_of(chunk, half):
        return pl.multiple_of(target_lat(chunk, 1) * NLON + 8 * half, 8)

    @pl.when(comp == 0)
    def _():
        loads[0].start()
        greet(1)
        loads[0].wait()
        for ch in range(2):
            for par in range(2):
                sa2[pl.ds(2 * ch + par, NT, stride=4), :] = f_ref[2 + ch, :, pl.ds(128 * par, 128)]
        def air(k, carry):
            rows = pl.ds(pl.multiple_of(8 * k, 8), 8)
            wx, wy, cx, cy, rho = (f_ref[i, rows, :] for i in (0, 1, 2, 3, 6))
            scale = rho * 0.1 * root(wx * wx + wy * wy + 1.0)
            outb[0, rows, :] = scale * wx
            outb[1, rows, :] = scale * wy
            rx = wx - cx
            ry = wy - cy
            speed = root(rx * rx + ry * ry + 1.0)
            scale = rho * (0.1 + 0.05 * speed) * speed
            opn[0, rows, :] = scale * rx
            opn[1, rows, :] = scale * ry
            return carry

        lax.fori_loop(0, 16, air, 0)


        for chunk in range(DIRECT):
            for half in range(2):
                base = rows_of(chunk, half)
                for par in range(2):
                    lanes = pl.ds(128 * par, 128)
                    for ch in range(2):
                        sd2[pl.ds(8 * base + 2 * ch + par, 8, stride=8), :] = outb[ch, pl.ds(base, 8), lanes]
                        sd2[pl.ds(8 * base + 4 + 2 * ch + par, 8, stride=8), :] = f_ref[4 + ch, pl.ds(base, 8), lanes]

        pl.semaphore_wait(barrier, NT)
        for chunk in range(DIRECT):
            send_chunk(sd, rd, sd_sem, rd_sem, chunk, 1, 8, 8)
        for chunk in range(NLAT):
            send_chunk(sa, ra, sa_sem, ra_sem, chunk, 1)

        for chunk in range(DIRECT, NLAT):
            wait_chunk(ra, ra_sem, chunk)

            for half in range(2):
                base = rows_of(chunk, half)
                rows = pl.ds(base, 8)
                for par in range(2):
                    lanes = pl.ds(128 * par, 128)
                    conc = ra2[pl.ds(4 * base + par, 8, stride=4), :]
                    mass = ra2[pl.ds(4 * base + 2 + par, 8, stride=4), :]
                    for ch in range(2):
                        sb2[pl.ds(4 * base + 2 * ch + par, 8, stride=4), :] = (
                            conc * outb[ch, rows, lanes] - mass * f_ref[4 + ch, rows, lanes]
                        )
            send_chunk(sb, rb, sb_sem, rb_sem, chunk, 1)

        for chunk in range(DIRECT):
            wait_chunk(ra, ra_sem, chunk, 2)
        for chunk in range(NLAT):
            wait_chunk(rb, rb_sem, chunk)
            base = rows_of(chunk, 0)
            rows = pl.ds(base, NLON)
            for par in range(2):
                lanes = pl.ds(128 * par, 128)
                rest = 1.0 - ra2[pl.ds(4 * base + par, NLON, stride=4), :]
                for ch in range(2):
                    out_ref[ch, rows, lanes] = (
                        rb2[pl.ds(4 * base + 2 * ch + par, NLON, stride=4), :] + rest * opn[ch, rows, lanes]
                    )
        wait_bytes(sa, sa_sem)
        wait_bytes(sb.at[pl.ds(0, 4 * NLON * (NLAT - DIRECT))], sb_sem)
        wait_bytes(sd.at[pl.ds(0, 8 * NLON * DIRECT)], sd_sem)

    east = lax.rem(lo + 1, NLON)
    west = lax.rem(lo + NLON - 1, NLON)
    has_south = la > 0
    has_north = la < NLAT - 1

    def halo_copies(group, bufs):
        ss, sn, hs, hn, se, sw, pw, pe = bufs
        size = se.shape[0]
        south, north = la - 1, la + 1
        first, last = pl.ds(0, 8), pl.ds(size - 8, 8)
        below, middle, above = pl.ds(0, 8), pl.ds(8, size), pl.ds(8 + size, 8)
        plan = (
            (None, se, pw.at[middle], la, east),
            (None, sw, pe.at[middle], la, west),
            (has_north, sn, hs, north, lo),
            (has_north, se.at[last], pw.at[below], north, east),
            (has_north, sw.at[last], pe.at[below], north, west),
            (has_south, ss, hn, south, lo),
            (has_south, se.at[first], pw.at[above], south, east),
            (has_south, sw.at[first], pe.at[above], south, west),
        )
        return [
            (
                cond,
                pltpu.make_async_remote_copy(
                    src_ref=src, dst_ref=dst, send_sem=h_send.at[8 * group + n], recv_sem=h_recv.at[8 * group + n],
                    device_id=(1, tla, tlo), device_id_type=MESH,
                ),
            )
            for n, (cond, src, dst, tla, tlo) in enumerate(plan)
        ]

    def under(cond, action):
        if cond is None:
            action()
        else:
            pl.when(cond)(action)

    def halo_start(group, bufs, source):
        ss, sn, hs, hn, se, sw, pw, pe = bufs
        count, size = ss.shape[0], se.shape[0]
        for n in range(count):
            ss[n] = source(n)[pl.ds(0, 2), :]
            sn[n] = source(n)[pl.ds(126, 2), :]
        lane = lanes_of((size, 128))
        to_east = jnp.zeros((size, 128), F32)
        to_west = to_east
        for g in range(NT // size):
            for n in range(count):
                for par in range(2):
                    at = 8 * count * g + 8 * n + 4 * par
                    value = source(n)[pl.ds(size * g, size), pl.ds(128 * par, 128)]
                    here = (lane >= at) & (lane < at + 4)
                    to_west = jnp.where(here, pltpu.roll(value, at, 1) if at else value, to_west)
                    to_east = jnp.where(here, pltpu.roll(value, (at - 124) % 128, 1) if at != 124 else value, to_east)
        se[...] = to_east
        sw[...] = to_west
        for cond, copy in halo_copies(group, bufs):
            under(cond, copy.start)

    def halo_walls(bufs):
        ss, sn, hs, hn, se, sw, pw, pe = bufs
        size = se.shape[0]
        zero = jnp.zeros((8, 128), F32)

        @pl.when(la == 0)
        def _():
            hs[...] = jnp.zeros(hs.shape, F32)
            pw[pl.ds(0, 8), :] = zero
            pe[pl.ds(0, 8), :] = zero

        @pl.when(la == NLAT - 1)
        def _():
            hn[...] = jnp.zeros(hn.shape, F32)
            pw[pl.ds(8 + size, 8), :] = zero
            pe[pl.ds(8 + size, 8), :] = zero

    def halo_main(channels, source):
        for n, channel in enumerate(channels):
            for par in range(2):
                x[2 * channel + par, pl.ds(TOP, NT), pl.ds(0, 128)] = source(n)[:, pl.ds(128 * par, 128)]

    def halo_finish(group, bufs, channels):
        ss, sn, hs, hn, se, sw, pw, pe = bufs
        count, size = ss.shape[0], se.shape[0]
        copies = halo_copies(group, bufs)
        received = {2: has_south, 3: has_south, 4: has_south, 5: has_north, 6: has_north, 7: has_north}
        for n, (cond, copy) in enumerate(copies):
            under(received.get(n), copy.wait_recv)
        groups = NT // size
        parts = [(TOP + size * g, size, 8, g) for g in range(groups)]
        parts += [(8, 8, 0, groups - 1), (TOP + NT, 8, 8 + size, 0)]
        for start, rows, at, g in parts:
            from_west = pw[pl.ds(at, rows), :]
            from_east = pe[pl.ds(at, rows), :]
            lane = lanes_of((rows, 128))
            for n, channel in enumerate(channels):
                for par in range(2):
                    j = 8 * count * g + 8 * n + 4 * par
                    right = pltpu.roll(from_east, 128 - j, 1) if j else from_east
                    left = pltpu.roll(from_west, 124 - j, 1) if j != 124 else from_west
                    x[2 * channel + par, pl.ds(start, rows), pl.ds(128, 128)] = jnp.where(lane < 64, right, left)
        for n, channel in enumerate(channels):
            for par in range(2):
                lanes = pl.ds(128 * par, 128)
                x[2 * channel + par, pl.ds(TOP - 2, 2), pl.ds(0, 128)] = hs[n, :, lanes]
                x[2 * channel + par, pl.ds(TOP + NT, 2), pl.ds(0, 128)] = hn[n, :, lanes]

    def halo_sent(group, bufs):
        for cond, copy in halo_copies(group, bufs):
            under(cond, copy.wait_send)

    ice_bufs = (ss1, sn1, hs1, hn1, se1, sw1, pw1, pe1)
    sea_bufs = (ss2, sn2, hs2, hn2, se2, sw2, pw2, pe2)

    @pl.when(comp == 1)
    def _():
        for load in loads:
            load.start()
        greet(0)
        greet(1)
        for chunk in range(NLAT):
            first = lax.rem(la + chunk, NLAT) * NLON
            if chunk < DIRECT:
                rb[pl.ds(4 * first, 4 * NLON)] = jnp.zeros((4 * NLON, 1, 128), F32)
            else:
                rd[pl.ds(8 * first, 8 * NLON)] = jnp.zeros((8 * NLON, 1, 128), F32)
        for load in loads:
            load.wait()
        square = (NT, NT)
        diagonal = lax.broadcasted_iota(jnp.int32, square, 0) == lanes_of(square)
        covered = jnp.sum(jnp.where(diagonal, cov_ref[...].astype(F32), 0.0), axis=1, keepdims=True)
        act[...] = covered * (1 - land_ref[...]).astype(F32)
        halo_walls(ice_bufs)
        halo_walls(sea_bufs)

        pl.semaphore_wait(barrier, 2 * NT)

        def tell_one(tla, tlo):
            pltpu.make_async_remote_copy(
                src_ref=own_ref, dst_ref=ids.at[me], send_sem=id_send, recv_sem=id_recv,
                device_id=(1, tla, tlo), device_id_type=MESH,
            ).start()

        for tlo in others[1:]:
            tell_one(la, tlo)

        def tell(k, carry):
            tla = lax.rem(la + k, NLAT)
            for tlo in others:
                tell_one(tla, tlo)
            return carry

        lax.fori_loop(1, NLAT, tell, 0)
        ids[me] = own_ref[...]

        def ice_source(n):
            return f_ref.at[n] if n < 7 else act

        halo_start(0, ice_bufs, ice_source)

        wait_bytes(ids.at[pl.ds(0, NT - 1)], id_recv)
        every = ids.reshape(NT, NT)[...]
        local = jnp.where(lanes_of(square) == me, (every - NT * me).astype(F32), 0.0)
        local = jnp.sum(local, axis=1, keepdims=True)
        q = (local == lanes_of(square).astype(F32)).astype(F32)
        qmat[0] = q
        qmat[1] = q.T

        def to_slots(values):
            return jnp.dot(qmat[0], values, precision=HIGHEST, preferred_element_type=F32)

        def to_blocks(values):
            return jnp.dot(qmat[1], values, precision=HIGHEST, preferred_element_type=F32)

        a = act[...]
        for ch, value in enumerate((f_ref[3] * a, f_ref[2] * a)):
            moved = to_slots(value)
            for par in range(2):
                sa2[pl.ds(2 * ch + par, NT, stride=4), :] = moved[:, 128 * par : 128 * par + 128]
        for chunk in range(DIRECT, NLAT):
            send_chunk(sa, ra, sa_sem, ra_sem, chunk, 0)
        for chunk in range(DIRECT):
            send_chunk(sa, ra, sa_sem, ra_sem, chunk, 0, 4, 2)
        halo_main(GROUP_ICE, ice_source)
        halo_finish(0, ice_bufs, GROUP_ICE)

        def prepare(k, carry):
            rows = pl.ds(pl.multiple_of(48 * k + 8, 8), 48)
            for par in range(2):
                conc = x[2 * DRAG + par, rows, :]
                active = x[2 * ACT + par, rows, :]
                mass = x[2 * MASS + par, rows, :]
                x[2 * STR + par, rows, :] = mass * jnp.exp(2.0 * (conc - 1.0)) * (active * (1.0 / 6.0))
                x[2 * DRAG + par, rows, :] = 1.5 * conc * active
                x[2 * DEN + par, rows, :] = 2.0 * jnp.maximum(mass, 0.5)
                x[2 * TURN + par, rows, :] = 0.3 * mass
                x[2 * MASS + par, rows, :] = 2.0 * mass
                one = 0.5 * x[2 * S1 + par, rows, :]
                two = 0.5 * x[2 * S2 + par, rows, :]
                x[2 * S1 + par, rows, :] = one + two
                x[2 * S2 + par, rows, :] = one - two
            return carry

        lax.fori_loop(0, 3, prepare, 0)

        third = 1.0 / 1.5
        both = pl.ds(0, 256)

        def stress():
            for r in (8, 80):
                for par in range(2):
                    def get(channel, p=par, row=r):
                        return x[2 * channel + p, pl.ds(row, 72), :]

                    u, v = get(U), get(V)
                    un, vn = (get(c, 1) if par == 0 else get(c, 0, r + 1) for c in (U, V))
                    sxx = pltpu.roll(u, 255, 1) - u
                    syy = vn - v
                    shear = (un - u) + (pltpu.roll(v, 255, 1) - v)
                    div = sxx + syy
                    ten = sxx - syy
                    strength = get(STR)
                    visc = strength * lax.rsqrt(div * div + (ten * ten + shear * shear + 1.0) * 0.25)
                    quarter = 0.25 * visc
                    total = visc * div - strength
                    differ = quarter * ten
                    rows = pl.ds(r, 72)
                    x[2 * S1 + par, rows, :] = get(S1) * third + (total + differ)
                    x[2 * S2 + par, rows, :] = get(S2) * third + (total - differ)
                    x[2 * S12 + par, rows, :] = get(S12) * third + quarter * shear

        def momentum(r, n, half, final=False):
            lanes = both if half is None else pl.ds(128 * half, 128)
            for par in range(2):
                def get(channel, p=par, row=r, where=lanes):
                    return x[2 * channel + p, pl.ds(row, n), where]

                def west_of(channel):
                    rolled = pltpu.roll(get(channel), 1, 1)
                    if half is None:
                        return rolled
                    beyond = pltpu.roll(get(channel, where=pl.ds(128 - 128 * half, 128)), 1, 1)
                    return jnp.where(lanes_of((n, 128)) == 0, beyond, rolled)

                s12 = get(S12)
                south = (1, r - 1) if par == 0 else (0, r)
                force_x = get(S1) - west_of(S1) + (s12 - get(S12, *south))
                force_y = s12 - west_of(S12) + (get(S2) - get(S2, *south))
                u, v, cx, cy, mass2, turn = (get(c) for c in (U, V, CX, CY, MASS, TURN))
                dx = cx - u
                dy = cy - v
                base = get(DRAG)
                drag = base * root(dx * dx + dy * dy + 0.1)
                scale = get(ACT) / (get(DEN) + drag)
                unew = scale * (mass2 * u + force_x + get(PX) + drag * cx + turn * v)
                vnew = scale * (mass2 * v + force_y + get(PY) + drag * cy - turn * u)
                if final:
                    rows, place = pl.ds(r - TOP, n), pl.ds(128 * par, 128)
                    out_ref[0, rows, place] = unew
                    out_ref[1, rows, place] = vnew
                    dx = unew - cx
                    dy = vnew - cy
                    factor = base * root(dx * dx + dy * dy + 0.1)
                    gat[0, rows, place] = factor * dx
                    gat[1, rows, place] = factor * dy
                else:
                    x[2 * U + par, pl.ds(r, n), lanes] = unew
                    x[2 * V + par, pl.ds(r, n), lanes] = vnew

        stress()

        for chunk in range(NLAT):
            wait_chunk(ra, ra_sem, chunk)
        for ch in range(2):
            for par in range(2):
                gat[ch, :, pl.ds(128 * par, 128)] = to_blocks(ra2[pl.ds(2 * ch + par, NT, stride=4), :])
        for chunk in range(DIRECT):
            wait_chunk(rd, rd_sem, chunk, 8)
        for par in range(2):
            lanes = pl.ds(128 * par, 128)
            for ch in range(2):
                stress_of_air = to_blocks(rd2[pl.ds(2 * ch + par, NT, stride=8), :])
                tilt = to_blocks(rd2[pl.ds(4 + 2 * ch + par, NT, stride=8), :])
                gat[2 + ch, :, lanes] = act[:, lanes] * (f_ref[3, :, lanes] * stress_of_air - f_ref[2, :, lanes] * tilt)
        for chunk in range(DIRECT, NLAT):
            wait_chunk(rb, rb_sem, chunk)
        for ch in range(2):
            for par in range(2):
                gat[2 + ch, :, pl.ds(128 * par, 128)] += to_blocks(rb2[pl.ds(2 * ch + par, NT, stride=4), :])
        halo_start(1, sea_bufs, lambda n: gat.at[n])
        halo_main(GROUP_SEA, lambda n: gat.at[n])
        momentum(TOP, 64, 0)
        momentum(TOP + 64, 64, 0)
        halo_finish(1, sea_bufs, GROUP_SEA)
        momentum(8, 8, 0)
        momentum(TOP + NT, 8, 0)
        momentum(8, 144, 1)
        for repeat in range(NSUB - 2):
            stress()
            momentum(8, 72, None)
            momentum(80, 72, None)
        stress()
        momentum(TOP, 64, 0, True)
        momentum(TOP + 64, 64, 0, True)
        for ch in range(2):
            for par in range(2):
                sb2[pl.ds(2 * ch + par, NT, stride=4), :] = to_slots(gat[ch, :, pl.ds(128 * par, 128)])
        for chunk in range(NLAT):
            send_chunk(sb, rb, sb_sem, rb_sem, chunk, 0)
        wait_bytes(ids.at[pl.ds(0, NT - 1)], id_send)
        for group, bufs in enumerate((ice_bufs, sea_bufs)):
            halo_sent(group, bufs)
        wait_bytes(sa.at[pl.ds(0, 4 * NT - 2 * NLON * DIRECT)], sa_sem)
        wait_bytes(sb, sb_sem)


def halo_scratch(count):
    size = 16 * count // 2
    return [
        *[pltpu.VMEM((count, 2, 256), F32)] * 4,
        *[pltpu.VMEM((size, 128), F32)] * 2,
        *[pltpu.VMEM((size + 16, 128), F32)] * 2,
    ]


def per_device(fields, block_owner, ice_covered, land_mask):
    out = pl.pallas_call(
        kernel,
        out_shape=jax.ShapeDtypeStruct((2, NT, 256), F32),
        in_specs=[pl.BlockSpec(memory_space=pltpu.HBM)] * 4,
        out_specs=pl.BlockSpec(memory_space=pltpu.VMEM),
        scratch_shapes=[
            pltpu.VMEM((7, NT, 256), F32),
            pltpu.VMEM((1, NT), jnp.int32),
            pltpu.VMEM((1, NT), jnp.int32),
            pltpu.VMEM((NT, 256), jnp.int32),
            pltpu.SemaphoreType.DMA((4,)),
            pltpu.VMEM((NT, 1, NT), jnp.int32),
            *[pltpu.VMEM((4 * NT, 1, 128), F32)] * 4,
            *[pltpu.VMEM((8 * NT, 1, 128), F32)] * 2,
            pltpu.VMEM((30, ROWS, 256), F32),
            pltpu.VMEM((NT, 256), F32),
            pltpu.VMEM((4, NT, 256), F32),
            pltpu.VMEM((2, NT, 256), F32),
            pltpu.VMEM((2, NT, 256), F32),
            pltpu.VMEM((2, NT, NT), F32),
            *halo_scratch(8),
            *halo_scratch(4),
            pltpu.SemaphoreType.DMA,
            pltpu.SemaphoreType.DMA,
            pltpu.SemaphoreType.DMA,
            pltpu.SemaphoreType.DMA((NLAT,)),
            pltpu.SemaphoreType.DMA,
            pltpu.SemaphoreType.DMA((NLAT,)),
            pltpu.SemaphoreType.DMA,
            pltpu.SemaphoreType.DMA((NLAT,)),
            pltpu.SemaphoreType.DMA((16,)),
            pltpu.SemaphoreType.DMA((16,)),
        ],
        compiler_params=pltpu.CompilerParams(
            collective_id=0, has_side_effects=True, vmem_limit_bytes=40 * 1024 * 1024
        ),
    )(
        *(
            pltpu.with_memory_space_constraint(a, pltpu.HBM)
            for a in (fields[0], block_owner.reshape(1, NT), ice_covered.reshape(1, NT), land_mask)
        )
    )
    return out[None]


def solution(mesh):
    placed = (
        P("comp", None, ("lat", "lon"), None),
        P(("lat", "lon")),
        P(("lat", "lon")),
        P(("lat", "lon"), None),
    )
    return jax.shard_map(
        per_device,
        mesh=mesh,
        in_specs=placed,
        out_specs=P("comp", None, ("lat", "lon"), None),
        check_vma=False,
    )
```
